16 devices in a mesh: rep: 4 (over y, z, core), dp: 4 (over x).
Axes of the slice: x: 4, y: 2, z: 1, core: 2. Of those that a mesh axis runs over, the one named last changes fastest.
The devices are a block of a 4x4x8 slice.
Arguments:
- x: bfloat16 [16, 4096, 768], P(('rep', 'dp')), parts along dimension 0
- dy: bfloat16 [16, 4096, 768], P(('rep', 'dp')), parts along dimension 0
- w_gate: bfloat16 [2, 768, 1792], replicated
- w_up: bfloat16 [2, 768, 1792], replicated
- w_down: bfloat16 [2, 1792, 768], replicated
- m_w_gate: float32 [2, 768, 1792], P(None, 'dp')
- m_w_up: float32 [2, 768, 1792], P(None, 'dp')
- m_w_down: float32 [2, 1792, 768], P(None, 'dp')
- v_w_gate: float32 [2, 768, 1792], P(None, 'dp')
- v_w_up: float32 [2, 768, 1792], P(None, 'dp')
- v_w_down: float32 [2, 1792, 768], P(None, 'dp')
Outputs:
- output 1: bfloat16 [8, 768, 1792], P('rep'), parts along dimension 0
- output 2: bfloat16 [8, 768, 1792], P('rep'), parts along dimension 0
- output 3: bfloat16 [8, 1792, 768], P('rep'), parts along dimension 0
- output 4: float32 [8, 768, 1792], P('rep', 'dp'), parts along dimension 0
- output 5: float32 [8, 768, 1792], P('rep', 'dp'), parts along dimension 0
- output 6: float32 [8, 1792, 768], P('rep', 'dp'), parts along dimension 0
- output 7: float32 [8, 768, 1792], P('rep', 'dp'), parts along dimension 0
- output 8: float32 [8, 768, 1792], P('rep', 'dp'), parts along dimension 0
- output 9: float32 [8, 1792, 768], P('rep', 'dp'), parts along dimension 0
There are 4 independent parts. The reference program is written for one: setup_inputs(seed, part) draws one part's arguments, and reference() takes and returns one part's arrays. A program takes and returns all parts, laid end to end along the dimension named above; an argument that names none is the same for every part.
All inputs are finite; a program needn't handle non-finite values.
Results may differ from the reference program's by a relative error of at most 0.022.
Values are sent between devices in bfloat16 or wider.
A program may use at most 768 MiB of HBM per device.

```python
import jax
import jax.numpy as jnp
from jax import lax

SEQUENCES = 4
TOKENS = 4096
D = 768
FF = 1792
LAYERS = 2
NAMES = ("w_gate", "w_up", "w_down")
SHAPES = {"w_gate": (LAYERS, D, FF), "w_up": (LAYERS, D, FF), "w_down": (LAYERS, FF, D)}


def bump(key, n, height):
    away = (jnp.arange(n, dtype=jnp.int32) - jax.random.randint(key, (), 0, n, jnp.int32)) % n
    return jnp.where(away < n // 8, height, 1.0)


def together(key, own, strength):
    shared = jax.random.normal(key, own.shape[1:], jnp.float32)
    return (own + strength * shared) * lax.rsqrt(1 + strength * strength)


def setup_inputs(seed: int = 0, part: int = 0) -> dict:
    kx, kdy, ka, kb, kz, kf, kh, kl, *keys = jax.random.split(jax.random.key(seed), 8 + 3 * len(NAMES))
    kx, kdy, ka, kb = (jax.random.fold_in(k, part) for k in (kx, kdy, ka, kb))
    kw, km, kv = (keys[i::3] for i in range(3))
    shape = (SEQUENCES, TOKENS, D)
    much_x, much_dy = jax.random.uniform(kz, (2,), jnp.float32, 0.0, 1.0)
    loud = 2.0 ** jax.random.uniform(jax.random.fold_in(kz, 1), (), jnp.float32, -1.0, 2.0)
    layers = 2.0 ** jax.random.uniform(kl, (LAYERS, 1, 1), jnp.float32, -1.0, 1.0)
    x = together(ka, jax.random.normal(kx, shape, jnp.float32), much_x) * bump(kf, D, 4.0)
    dy = together(kb, jax.random.normal(kdy, shape, jnp.float32), much_dy)
    drawn = {"x": x.astype(jnp.bfloat16), "dy": (loud * dy * (SEQUENCES * TOKENS) ** -0.5).astype(jnp.bfloat16)}
    for key, name in zip(kw, NAMES, strict=True):
        w = jax.random.normal(key, SHAPES[name], jnp.float32) * SHAPES[name][1] ** -0.5
        drawn[name] = (w * {"w_gate": 1.0, "w_up": bump(kh, FF, 4.0), "w_down": layers}[name]).astype(jnp.bfloat16)
    for key, name in zip(km, NAMES, strict=True):
        drawn[f"m_{name}"] = 0.1 * jax.random.normal(key, SHAPES[name], jnp.float32)
    for key, name in zip(kv, NAMES, strict=True):
        drawn[f"v_{name}"] = jax.random.uniform(key, SHAPES[name], jnp.float32, 0.005, 0.015)
    return drawn


def matmul(a, w):
    return jnp.dot(a, w, preferred_element_type=jnp.float32).astype(jnp.bfloat16)


def normed(h):
    wide = h.astype(jnp.float32)
    scale = lax.rsqrt(jnp.mean(wide**2, -1, keepdims=True) + 1e-6)
    return (wide * scale).astype(jnp.bfloat16)


def layer(h, w):
    a = normed(h)
    gate = jnp.dot(a, w["w_gate"], preferred_element_type=jnp.float32)
    up = jnp.dot(a, w["w_up"], preferred_element_type=jnp.float32)
    return h + matmul((jax.nn.silu(gate) * up).astype(jnp.bfloat16), w["w_down"])


def adamw(w, m, v, g):
    m = 0.9 * m + 0.1 * g
    v = 0.95 * v + 0.05 * g * g
    step = m * lax.rsqrt(v + 1e-8) + 0.1 * w
    return (w - 0.02 * step).astype(jnp.bfloat16), m, v


def clipped(gradients, sum_of_squares, count):
    factor = jnp.minimum(1.0, 0.5 * lax.rsqrt(sum_of_squares / count + 1e-30))
    return [g * factor for g in gradients]


def stack(weights, h):
    return lax.scan(lambda h, w: (layer(h, w), None), h, weights)[0]


def reference(x, dy, w_gate, w_up, w_down, m_w_gate, m_w_up, m_w_down, v_w_gate, v_w_up, v_w_down):
    weights = dict(zip(NAMES, (w_gate, w_up, w_down), strict=True))

    def take(so_far, sequence):
        h, by_y = sequence
        _, back = jax.vjp(lambda w: stack(w, h), weights)
        return jax.tree.map(lambda total, term: total + term.astype(jnp.float32), so_far, back(by_y)[0]), None

    none_yet = {name: jnp.zeros(w.shape, jnp.float32) for name, w in weights.items()}
    by_weights, _ = lax.scan(take, none_yet, (x, dy))
    gradients = [by_weights[name].astype(jnp.bfloat16).astype(jnp.float32) for name in NAMES]
    gradients = clipped(gradients, sum(jnp.sum(g * g) for g in gradients), sum(g.size for g in gradients))
    new = [
        adamw(w.astype(jnp.float32), m, v, g)
        for w, m, v, g in zip((w_gate, w_up, w_down), (m_w_gate, m_w_up, m_w_down), (v_w_gate, v_w_up, v_w_down), gradients, strict=True)
    ]
    return tuple(one[which] for which in range(3) for one in new)
```

```python
import functools

import jax
import jax.numpy as jnp
from jax import lax
from jax.experimental import pallas as pl
from jax.experimental.pallas import tpu as pltpu
from jax.sharding import PartitionSpec as P

F32, BF16 = jnp.float32, jnp.bfloat16
VMEM_LIMIT = 66_000_000
CHUNK = 256
MESH = pl.DeviceIdType.MESH
ANY = pl.BlockSpec(memory_space=pl.ANY)


def dot(a, b):
    return jnp.dot(a, b, preferred_element_type=F32)


def dot_t(a, b):
    return lax.dot_general(a, b, (((1,), (1,)), ((), ())), preferred_element_type=F32)


def scale_of(wide):
    return lax.rsqrt(jnp.mean(wide * wide, -1, keepdims=True) + 1e-6)


def whole(shape, at=None):
    if at is None:
        return pl.BlockSpec(shape, lambda *_: (0,) * len(shape), pipeline_mode=pl.Buffered(1))
    return pl.BlockSpec((None, *shape), lambda *_: (at,) + (0,) * len(shape), pipeline_mode=pl.Buffered(1))


def ring():
    n = lax.axis_size("dp")
    me = lax.axis_index("dp")
    return me, (me + 1) % n, (me + n - 1) % n, (me + 2) % n


def meet(others):
    barrier = pltpu.get_barrier_semaphore()
    for other in others:
        pl.semaphore_signal(barrier, inc=1, device_id={"dp": other}, device_id_type=MESH)
    pl.semaphore_wait(barrier, len(others))


def remote(src, dst, send, recv, to):
    return pltpu.make_async_remote_copy(src_ref=src, dst_ref=dst, send_sem=send, recv_sem=recv, device_id={"dp": to}, device_id_type=MESH)


class Scatter:
    def __init__(self, piece, landed, final, send, recv):
        self.piece, self.landed, self.final = piece, landed, final
        self.me, right, left, far = ring()
        self.right, self.left = right, left
        self.routes = (
            lambda: (piece(far, 0), landed.at[0], right),
            lambda: (piece(far, 1), landed.at[1], left),
            lambda: (piece(right, 1), final.at[0, 1], right),
            lambda: (piece(left, 0), final.at[1, 0], left),
            lambda: (landed.at[0], final.at[0, 0], right),
            lambda: (landed.at[1], final.at[1, 1], left),
        )
        self.semaphores = send, recv

    def copy(self, k):
        src, dst, to = self.routes[k]()
        return remote(src, dst, self.semaphores[0].at[k], self.semaphores[1].at[k], to)

    def start(self):
        for k in range(4):
            self.copy(k).start()

    def middle(self):
        for k, own in enumerate((self.piece(self.right, 0), self.piece(self.left, 1))):
            self.copy(k).wait_recv()
            self.landed[k] = (self.landed[k].astype(F32) + own[...].astype(F32)).astype(BF16)
        for k in range(4, 6):
            self.copy(k).start()

    def finish(self, put):
        for k in range(2, 6):
            self.copy(k).wait_recv()
        for half in range(2):
            total = self.piece(self.me, half)[...].astype(F32) + self.final[0, half].astype(F32) + self.final[1, half].astype(F32)
            put(half, total.astype(BF16))
        for k in range(6):
            self.copy(k).wait_send()


def forward_body(x_ref, dy_ref, wg_ref, wu_ref, wd_ref, a_ref, at_ref, h_ref, a2_ref, a2t_ref, dyt_ref, hid):
    x = x_ref[...].astype(F32)
    a = (x * scale_of(x)).astype(BF16)
    a_ref[...] = a
    for j in range(wg_ref.shape[1] // CHUNK):
        at = slice(j * CHUNK, (j + 1) * CHUNK)
        gate, up = dot(a, wg_ref[:, at]), dot(a, wu_ref[:, at])
        hid[:, at] = (gate * jax.nn.sigmoid(gate) * up).astype(BF16)
    at_ref[...] = a.T
    dyt_ref[...] = dy_ref[...].T
    h = (x + dot(hid[...], wd_ref[...]).astype(BF16).astype(F32)).astype(BF16)
    h_ref[...] = h
    wide = h.astype(F32)
    a2 = (wide * scale_of(wide)).astype(BF16)
    a2_ref[...] = a2
    a2t_ref[...] = a2.T


def forward(x, dy, wg, wu, wd, layer, tile=512):
    tokens, d = x.shape
    ff = wg.shape[2]
    rows = pl.BlockSpec((tile, d), lambda i: (i, 0))
    columns = pl.BlockSpec((d, tile), lambda i: (0, i))
    flat, turned = jax.ShapeDtypeStruct((tokens, d), BF16), jax.ShapeDtypeStruct((d, tokens), BF16)
    return pl.pallas_call(
        forward_body,
        grid=(tokens // tile,),
        in_specs=[rows, rows, whole((d, ff), layer), whole((d, ff), layer), whole((ff, d), layer)],
        out_specs=[rows, columns, rows, rows, columns, columns],
        out_shape=[flat, turned, flat, flat, turned, turned],
        scratch_shapes=[pltpu.VMEM((tile, ff), BF16)],
        compiler_params=pltpu.CompilerParams(vmem_limit_bytes=VMEM_LIMIT),
        cost_estimate=pl.CostEstimate(flops=6 * tokens * d * ff, bytes_accessed=16 * tokens * d, transcendentals=tokens * ff),
        name="forward",
    )(x, dy, wg, wu, wd)


def of(n):
    return lambda i: (2 * i) % n


def backward_body(tile, last, a_ref, at_ref, dy_ref, dyt_ref, wg_ref, wu_ref, wd_ref, *rest):
    if last:
        h_ref, dh_ref, dht_ref, gg, gu, gd, pair, down, gw, uw, dw, da, *comm = rest
    else:
        gg_in, gu_in, gd_in, pair_in, down_in, gg, gu, gd, pair, down, gw, uw, dw, *comm = rest
    landed, final, send, recv = comm[:4]
    landed1, final1, landed2, final2, send_d, recv_d = comm[4:10]
    tokens, d = a_ref.shape
    i, chunks = pl.program_id(0), down.shape[0] // CHUNK
    c = of(chunks)(i)
    me, right, left, far = ring()
    wide_rows, tall_rows = gg.shape[1], gd.shape[1]
    layer = 1 if last else 0

    def columns(number):
        return pl.ds(pl.multiple_of(of(chunks)(number) * CHUNK, CHUNK), CHUNK)

    def for_pair(ref, slot):
        def piece(owner, half):
            return ref.at[:, pl.ds(pl.multiple_of(owner * wide_rows + half * (wide_rows // 2), 32), wide_rows // 2), :]

        return Scatter(piece, landed.at[slot], final.at[slot], send.at[slot], recv.at[slot])

    def put_pair(layer, number):
        def put(half, value):
            rows = slice(half * (wide_rows // 2), (half + 1) * (wide_rows // 2))
            gg[layer, rows, columns(number)] = value[0]
            gu[layer, rows, columns(number)] = value[1]

        return put

    def for_down_1():
        def piece(owner, half):
            return down.at[pl.ds(pl.multiple_of(owner * 2 * CHUNK + half * (CHUNK // 2), 32), CHUNK // 2), :]

        return Scatter(piece, landed1, final1, send_d.at[0], recv_d.at[0])

    def put_down_1(half, value):
        gd[layer, pl.ds(pl.multiple_of(me * (2 * CHUNK - tall_rows) + half * (CHUNK // 2), 32), CHUNK // 2), :] = value

    short = 2 * CHUNK - tall_rows

    def start_2(owner, b):
        return b * short + (1 - (owner - b + 3) // 4) * CHUNK

    def for_down_2(ref, slot, b):
        def piece(owner, half):
            return ref.at[pl.ds(pl.multiple_of(owner * tall_rows + start_2(owner, b) + half * (short // 2), 32), short // 2), :]

        return Scatter(piece, landed2.at[slot, b], final2.at[slot, b], send_d.at[1 + 3 * slot + b], recv_d.at[1 + 3 * slot + b])

    def put_down_2(layer, b):
        def put(half, value):
            gd[layer, pl.ds(pl.multiple_of(start_2(me, b) + half * (short // 2), 32), short // 2), :] = value

        return put

    wg, wu, wd = wg_ref[...], wu_ref[...], wd_ref[...]

    def step(t, first):
        rows = pl.ds(t * tile if isinstance(t, int) else pl.multiple_of(t * tile, tile), tile)
        a, dy = a_ref[rows, :], dy_ref[rows, :]
        gate, up, dhid = dot(a, wg), dot(a, wu), dot_t(dy, wd).astype(BF16).astype(F32)
        sig = jax.nn.sigmoid(gate)
        silu = gate * sig
        hid = (silu * up).astype(BF16)
        dup = (dhid * silu).astype(BF16)
        dgate = (dhid * up * (sig + silu * (1 - sig))).astype(BF16)
        at, dyt = at_ref[:, rows], dyt_ref[:, rows]
        for total, term in ((dw, dot(dyt, hid)), (uw, dot(at, dup)), (gw, dot(at, dgate))):
            total[...] = term if first else total[...] + term
        if last:
            da_t = dot_t(dgate, wg) + dot_t(dup, wu)

            @pl.when(i == 0)
            def _():
                da[rows, :] = da_t

            @pl.when(i > 0)
            def _():
                da[rows, :] += da_t

    def steps(start, stop):
        lax.fori_loop(start, stop, lambda t, carry: (step(t, False), carry)[1], 0)

    @pl.when(i == 0)
    def _():
        meet((right, left))
        if not last:
            for_pair(pair_in, chunks).start()
            gg[1] = gg_in[1]
            gu[1] = gu_in[1]
            gd[1] = gd_in[1]

    @pl.when(i > 0)
    def _():
        for_pair(pair, i - 1).start()

    half = tokens // tile // 2
    step(0, True)
    steps(1, half)

    @pl.when(i > 0)
    def _():
        for_pair(pair, i - 1).middle()

    @pl.when(i == 4)
    def _():
        for_down_1().start()

    @pl.when(i == 5)
    def _():
        for_down_1().middle()

    @pl.when(i == 6)
    def _():
        for_down_1().finish(put_down_1)

    if not last:

        @pl.when(i == 0)
        def _():
            for_pair(pair_in, chunks).middle()
            for b in range(3):
                for_down_2(down_in, 0, b).start()

        @pl.when(i == 1)
        def _():
            for b in range(3):
                for_down_2(down_in, 0, b).middle()

        @pl.when(i == 2)
        def _():
            for b in range(3):
                for_down_2(down_in, 0, b).finish(put_down_2(1, b))

    steps(half, 2 * half)

    if not last:

        @pl.when(i == 0)
        def _():
            for_pair(pair_in, chunks).finish(put_pair(1, chunks - 1))

    @pl.when(i > 0)
    def _():
        for_pair(pair, i - 1).finish(put_pair(layer, i - 1))

    pair[0] = gw[...].astype(BF16)
    pair[1] = uw[...].astype(BF16)
    down[pl.ds(pl.multiple_of(c * CHUNK, CHUNK), CHUNK), :] = dw[...].astype(BF16).T

    @pl.when(i == chunks - 1)
    def _():
        if last:

            def finish(h_tile, dh_tile, dht_tile):
                t = pl.program_id(0)
                rows = pl.ds(pl.multiple_of(t * tile, tile), tile)
                wide = h_tile[...].astype(F32)
                scale = scale_of(wide)
                back = da[rows, :].astype(BF16).astype(F32)
                coefficient = jnp.sum(back * wide, -1, keepdims=True) * (scale * scale * scale) * (1.0 / wide.shape[1])
                through = (back * scale - wide * coefficient).astype(BF16)
                dh = (dy_ref[rows, :].astype(F32) + through.astype(F32)).astype(BF16)
                dh_tile[...] = dh
                dht_tile[...] = dh.T

            by_rows = pl.BlockSpec((tile, d), lambda t: (t, 0))
            by_columns = pl.BlockSpec((d, tile), lambda t: (0, t))
            pltpu.emit_pipeline(finish, grid=(tokens // tile,), in_specs=[by_rows], out_specs=[by_rows, by_columns])(h_ref, dh_ref, dht_ref)
        else:
            jobs = [(for_pair(pair, chunks - 1), put_pair(0, chunks - 1))]
            jobs += [(for_down_2(down, 1, b), put_down_2(0, b)) for b in range(3)]
            for job, _ in jobs:
                job.start()
            for job, _ in jobs:
                job.middle()
            for job, put in jobs:
                job.finish(put)


def backward(a, at, dy, dyt, wg, wu, wd, layer, h=None, before=None, group=4, tile=512):
    tokens, d = a.shape
    layers, _, ff = wg.shape
    last = h is not None
    chunks = ff // CHUNK
    flat, turned = whole((tokens, d)), whole((d, tokens))
    by_columns = pl.BlockSpec((None, d, CHUNK), lambda i: (layer, 0, of(chunks)(i)))
    by_rows = pl.BlockSpec((None, CHUNK, d), lambda i: (layer, of(chunks)(i), 0))
    shapes = (layers, d // group, ff), (layers, d // group, ff), (layers, ff // group, d), (2, d, CHUNK), (ff, d)
    out_specs = [whole(s) for s in shapes]
    out_shape = [jax.ShapeDtypeStruct(s, BF16) for s in shapes]
    scratch = [pltpu.VMEM((d, CHUNK), F32)] * 3
    extra, extra_specs = (), []
    if last:
        out_specs = [ANY, ANY] + out_specs
        out_shape = [jax.ShapeDtypeStruct((tokens, d), BF16), jax.ShapeDtypeStruct((d, tokens), BF16)] + out_shape
        scratch += [pltpu.VMEM((tokens, d), F32)]
        extra, extra_specs = (h,), [ANY]
    else:
        extra, extra_specs = before, [whole(s) for s in shapes]
    slots = chunks + 1
    short = 2 * CHUNK - ff // group
    dma = pltpu.SemaphoreType.DMA
    scratch += [
        pltpu.VMEM((slots, 2, 2, d // group // 2, CHUNK), BF16),
        pltpu.VMEM((slots, 2, 2, 2, d // group // 2, CHUNK), BF16),
        dma((slots, 6)),
        dma((slots, 6)),
        pltpu.VMEM((2, CHUNK // 2, d), BF16),
        pltpu.VMEM((2, 2, CHUNK // 2, d), BF16),
        pltpu.VMEM((2, 3, 2, short // 2, d), BF16),
        pltpu.VMEM((2, 3, 2, 2, short // 2, d), BF16),
        dma((7, 6)),
        dma((7, 6)),
    ]
    return pl.pallas_call(
        functools.partial(backward_body, tile, last),
        grid=(chunks,),
        in_specs=[flat, turned, flat, turned, by_columns, by_columns, by_rows] + extra_specs,
        out_specs=out_specs,
        out_shape=out_shape,
        scratch_shapes=scratch,
        compiler_params=pltpu.CompilerParams(vmem_limit_bytes=VMEM_LIMIT, collective_id=1 if last else 2, has_side_effects=True),
        cost_estimate=pl.CostEstimate(flops=(16 if last else 12) * tokens * d * ff, bytes_accessed=16 * tokens * d, transcendentals=tokens * ff),
        name="backward_last" if last else "backward_first",
    )(a, at, dy, dyt, wg, wu, wd, *extra)


def adamw(w, m, v, g):
    m = 0.9 * m + 0.1 * g
    v = 0.95 * v + 0.05 * g * g
    step = m * lax.rsqrt(v + 1e-8) + 0.1 * w
    return (w - 0.02 * step).astype(BF16), m, v


def update_body(count, *refs):
    g, w, m, v, new_w, new_m, new_v = (refs[k : k + 3] for k in range(0, 21, 3))
    held_w, held_m, held_v = (refs[k : k + 3] for k in range(21, 30, 3))
    mine, sums, norm_send, norm_recv, load, store, send, recv = refs[30:]
    me, right, left, far = ring()
    layers = g[0].shape[0]
    loads = {}
    for k in range(3):
        size = g[k].shape[1]
        for layer in range(layers):
            own = w[k].at[layer, pl.ds(pl.multiple_of(me * size, 32), size), :]
            for which, (src, dst) in enumerate(((own, held_w[k].at[layer]), (m[k].at[layer], held_m[k].at[layer]), (v[k].at[layer], held_v[k].at[layer]))):
                loads[k, layer, which] = pltpu.make_async_copy(src, dst, load.at[k, layer, which])
                loads[k, layer, which].start()
    meet((right, left, far))
    total = jnp.float32(0)
    for k in range(3):
        for layer in range(layers):

            def add(r, squares):
                part = g[k][layer, pl.ds(pl.multiple_of(r * 16, 16), 16), :].astype(F32)
                return squares + part * part

            total += jnp.sum(lax.fori_loop(0, g[k].shape[1] // 16, add, jnp.zeros((16, g[k].shape[2]), F32)))
    mine[...] = jnp.full(mine.shape, total, F32)
    sums[me] = mine[...]
    tells = [remote(mine, sums.at[me], norm_send.at[n], norm_recv.at[n], to) for n, to in enumerate((right, left, far))]
    for tell in tells:
        tell.start()
    for tell in tells:
        tell.wait()
    squares = sum(sums[n] for n in range(sums.shape[0]))
    factor = jnp.minimum(1.0, 0.5 * lax.rsqrt(squares / count + 1e-30))[0:1, 0:1]

    copies = []
    for k in range(3):
        size, rows = g[k].shape[1], 32
        half = size // 2
        for layer in range(layers):
            for which in range(3):
                loads[k, layer, which].wait()

            def change(r, carry):
                at = (layer, pl.ds(pl.multiple_of(r * rows, rows), rows), slice(None))
                new = adamw(held_w[k][at].astype(F32), held_m[k][at], held_v[k][at], g[k][at].astype(F32) * factor)
                held_w[k][at], held_m[k][at], held_v[k][at] = new
                return carry

            lax.fori_loop(0, size // rows, change, 0)

            def block(owner, start, length):
                return new_w[k].at[layer, pl.ds(pl.multiple_of(owner * size + start, 32), length), :]

            own, s, r = held_w[k].at[layer], send.at[k, layer], recv.at[k, layer]
            direct = [remote(own, block(me, 0, size), s.at[n], r.at[n], to) for n, to in enumerate((right, left))]
            on = [
                remote(block(left, 0, half), block(left, 0, half), s.at[2], r.at[2], right),
                remote(block(right, half, half), block(right, half, half), s.at[3], r.at[3], left),
            ]
            keep = [pltpu.make_async_copy(own, block(me, 0, size), store.at[k, layer, 0])]
            for which, (held, new) in enumerate(((held_m, new_m), (held_v, new_v))):
                keep.append(pltpu.make_async_copy(held[k].at[layer], new[k].at[layer], store.at[k, layer, 1 + which]))
            for copy in direct + keep:
                copy.start()
            copies.append((direct, on, keep))
    for direct, on, keep in copies:
        for first, second in zip(direct, on, strict=True):
            first.wait_recv()
            second.start()
    for direct, on, keep in copies:
        for copy in on:
            copy.wait()
        for copy in direct:
            copy.wait_send()
        for copy in keep:
            copy.wait()


def update(g, w, m, v):
    count = sum(t.size for t in w)
    layers = w[0].shape[0]
    shapes = [jax.ShapeDtypeStruct(t.shape, t.dtype) for t in (*w, *m, *v)]
    dma = pltpu.SemaphoreType.DMA
    group = w[0].shape[1] // m[0].shape[1]
    vmem = pl.BlockSpec(memory_space=pltpu.VMEM)
    return pl.pallas_call(
        functools.partial(update_body, count),
        in_specs=[vmem] * 3 + [ANY] * 9,
        out_specs=[ANY] * 9,
        out_shape=shapes,
        scratch_shapes=[pltpu.VMEM(t.shape, BF16) for t in m]
        + [pltpu.VMEM(t.shape, F32) for t in (*m, *v)]
        + [pltpu.VMEM((8, 128), F32), pltpu.VMEM((group, 8, 128), F32), dma((3,)), dma((3,))]
        + [dma((3, layers, 3)), dma((3, layers, 3)), dma((3, layers, 4)), dma((3, layers, 4))],
        compiler_params=pltpu.CompilerParams(vmem_limit_bytes=VMEM_LIMIT, collective_id=3, has_side_effects=True),
        name="update",
    )(*g, *w, *m, *v)


def solution(mesh):
    group = mesh.shape["dp"]

    def step(x, dy, *arrays):
        w, m, v = (arrays[i : i + 3] for i in (0, 3, 6))
        x, dy = x[0], dy[0]
        a1, a1t, h1, a2, a2t, dyt = forward(x, dy, *w, 0)
        dh, dht, *before = backward(a2, a2t, dy, dyt, *w, 1, h=h1, group=group)
        gg, gu, gd, *_ = backward(a1, a1t, dh, dht, *w, 0, before=before, group=group)
        return tuple(update((gg, gu, gd), w, m, v))

    sequence, rows = P(("rep", "dp"), None, None), P(None, "dp", None)
    return jax.shard_map(
        step,
        mesh=mesh,
        in_specs=(sequence,) * 2 + (P(),) * 3 + (rows,) * 6,
        out_specs=(P("rep", None, None),) * 3 + (P("rep", "dp", None),) * 6,
        check_vma=False,
    )
```

```python
import functools

import jax
import jax.numpy as jnp
from jax import lax
from jax.experimental import pallas as pl
from jax.experimental.pallas import tpu as pltpu
from jax.sharding import PartitionSpec as P

F32, BF16 = jnp.float32, jnp.bfloat16
VMEM_LIMIT = 66_000_000
CHUNK = 256
MESH = pl.DeviceIdType.MESH
ANY = pl.BlockSpec(memory_space=pl.ANY)


def dot(a, b):
    return jnp.dot(a, b, preferred_element_type=F32)


def dot_t(a, b):
    return lax.dot_general(a, b, (((1,), (1,)), ((), ())), preferred_element_type=F32)


def scale_of(wide):
    return lax.rsqrt(jnp.mean(wide * wide, -1, keepdims=True) + 1e-6)


def whole(shape, at=None):
    if at is None:
        return pl.BlockSpec(shape, lambda *_: (0,) * len(shape), pipeline_mode=pl.Buffered(1))
    return pl.BlockSpec((None, *shape), lambda *_: (at,) + (0,) * len(shape), pipeline_mode=pl.Buffered(1))


def ring():
    n = lax.axis_size("dp")
    me = lax.axis_index("dp")
    return me, (me + 1) % n, (me + n - 1) % n, (me + 2) % n


def meet(others):
    barrier = pltpu.get_barrier_semaphore()
    for other in others:
        pl.semaphore_signal(barrier, inc=1, device_id={"dp": other}, device_id_type=MESH)
    pl.semaphore_wait(barrier, len(others))


def remote(src, dst, send, recv, to):
    return pltpu.make_async_remote_copy(src_ref=src, dst_ref=dst, send_sem=send, recv_sem=recv, device_id={"dp": to}, device_id_type=MESH)


class Scatter:
    def __init__(self, piece, landed, final, send, recv):
        self.piece, self.landed, self.final = piece, landed, final
        self.me, right, left, far = ring()
        self.right, self.left = right, left
        self.routes = (
            lambda: (piece(far, 0), landed.at[0], right),
            lambda: (piece(far, 1), landed.at[1], left),
            lambda: (piece(right, 1), final.at[0, 1], right),
            lambda: (piece(left, 0), final.at[1, 0], left),
            lambda: (landed.at[0], final.at[0, 0], right),
            lambda: (landed.at[1], final.at[1, 1], left),
        )
        self.semaphores = send, recv

    def copy(self, k):
        src, dst, to = self.routes[k]()
        return remote(src, dst, self.semaphores[0].at[k], self.semaphores[1].at[k], to)

    def start(self):
        for k in range(4):
            self.copy(k).start()

    def middle(self):
        for k, own in enumerate((self.piece(self.right, 0), self.piece(self.left, 1))):
            self.copy(k).wait_recv()
            self.landed[k] = (self.landed[k].astype(F32) + own[...].astype(F32)).astype(BF16)
        for k in range(4, 6):
            self.copy(k).start()

    def finish(self, put):
        for k in range(2, 6):
            self.copy(k).wait_recv()
        for half in range(2):
            total = self.piece(self.me, half)[...].astype(F32) + self.final[0, half].astype(F32) + self.final[1, half].astype(F32)
            put(half, total.astype(BF16))
        for k in range(6):
            self.copy(k).wait_send()


def forward_body(x_ref, dy_ref, wg_ref, wu_ref, wd_ref, gate_ref, up_ref, at_ref, h_ref, a2_ref, a2t_ref, dyt_ref, hid):
    x = x_ref[...].astype(F32)
    a = (x * scale_of(x)).astype(BF16)
    for j in range(wg_ref.shape[1] // CHUNK):
        at = slice(j * CHUNK, (j + 1) * CHUNK)
        gate, up = dot(a, wg_ref[:, at]), dot(a, wu_ref[:, at])
        gate_ref[j], up_ref[j] = gate, up
        hid[:, at] = (gate * jax.nn.sigmoid(gate) * up).astype(BF16)
    at_ref[...] = a.T
    dyt_ref[...] = dy_ref[...].T
    h = (x + dot(hid[...], wd_ref[...]).astype(BF16).astype(F32)).astype(BF16)
    h_ref[...] = h
    wide = h.astype(F32)
    a2 = (wide * scale_of(wide)).astype(BF16)
    a2_ref[...] = a2
    a2t_ref[...] = a2.T


def forward(x, dy, wg, wu, wd, layer, tile=512):
    tokens, d = x.shape
    ff = wg.shape[2]
    chunks = ff // CHUNK
    rows = pl.BlockSpec((tile, d), lambda i: (i, 0))
    columns = pl.BlockSpec((d, tile), lambda i: (0, i))
    kept = pl.BlockSpec((chunks, tile, CHUNK), lambda i: (0, i, 0))
    flat, turned = jax.ShapeDtypeStruct((tokens, d), BF16), jax.ShapeDtypeStruct((d, tokens), BF16)
    by_chunk = jax.ShapeDtypeStruct((chunks, tokens, CHUNK), F32)
    return pl.pallas_call(
        forward_body,
        grid=(tokens // tile,),
        in_specs=[rows, rows, whole((d, ff), layer), whole((d, ff), layer), whole((ff, d), layer)],
        out_specs=[kept, kept, columns, rows, rows, columns, columns],
        out_shape=[by_chunk, by_chunk, turned, flat, flat, turned, turned],
        scratch_shapes=[pltpu.VMEM((tile, ff), BF16)],
        compiler_params=pltpu.CompilerParams(vmem_limit_bytes=VMEM_LIMIT),
        cost_estimate=pl.CostEstimate(flops=6 * tokens * d * ff, bytes_accessed=16 * tokens * d, transcendentals=tokens * ff),
        name="forward",
    )(x, dy, wg, wu, wd)


def of(n):
    return lambda i: (2 * i) % n


def backward_body(tile, unroll, last, *refs):
    if last:
        a_in, at_in, dy_in, dyt_in, wg_ref, wu_ref, wd_ref, h_ref, dh_ref, dht_ref, gg, gu, gd, pair, down, a_ref, *rest = refs
    else:
        gate_ref, up_ref, at_in, dy_in, dyt_in, wd_ref, gg_in, gu_in, gd_in, pair_in, down_in, gg, gu, gd, pair, down, *rest = refs
    at_ref, dy_ref, dyt_ref, loads, gw, uw, dw, landed, final, send, recv, landed1, final1, send_d, recv_d, *rest = rest
    if last:
        da, h, h_sem, out_sem = rest
    else:
        landed2, final2 = rest
    tokens, d = dy_ref.shape
    i, chunks = pl.program_id(0), down.shape[0] // CHUNK
    c = of(chunks)(i)
    me, right, left, far = ring()
    wide_rows, tall_rows = gg.shape[-2], gd.shape[-2]
    layer = () if last else (0,)

    def columns(number):
        return pl.ds(pl.multiple_of(of(chunks)(number) * CHUNK, CHUNK), CHUNK)

    def for_pair(ref, slot):
        def piece(owner, half):
            return ref.at[:, pl.ds(pl.multiple_of(owner * wide_rows + half * (wide_rows // 2), 32), wide_rows // 2), :]

        return Scatter(piece, landed.at[slot], final.at[slot], send.at[slot], recv.at[slot])

    def put_pair(layer, number):
        def put(half, value):
            rows = slice(half * (wide_rows // 2), (half + 1) * (wide_rows // 2))
            gg[(*layer, rows, columns(number))] = value[0]
            gu[(*layer, rows, columns(number))] = value[1]

        return put

    def for_down_1():
        def piece(owner, half):
            return down.at[pl.ds(pl.multiple_of(owner * 2 * CHUNK + half * (CHUNK // 2), 32), CHUNK // 2), :]

        return Scatter(piece, landed1, final1, send_d.at[0], recv_d.at[0])

    def put_down_1(half, value):
        gd[(*layer, pl.ds(pl.multiple_of(me * (2 * CHUNK - tall_rows) + half * (CHUNK // 2), 32), CHUNK // 2), slice(None))] = value

    short = 2 * CHUNK - tall_rows

    def start_2(owner, b):
        return b * short + (1 - (owner - b + 3) // 4) * CHUNK

    def for_down_2(ref, slot, b):
        def piece(owner, half):
            return ref.at[pl.ds(pl.multiple_of(owner * tall_rows + start_2(owner, b) + half * (short // 2), 32), short // 2), :]

        return Scatter(piece, landed2.at[slot, b], final2.at[slot, b], send_d.at[1 + 3 * slot + b], recv_d.at[1 + 3 * slot + b])

    def put_down_2(at, b):
        def put(half, value):
            gd[at, pl.ds(pl.multiple_of(start_2(me, b) + half * (short // 2), 32), short // 2), :] = value

        return put

    wd = wd_ref[...]
    if last:
        wg, wu = wg_ref[...], wu_ref[...]

    def rows_of(t):
        return pl.ds(pl.multiple_of(t * tile, tile), tile)

    def load(t):
        by_rows, by_columns = (rows_of(t), slice(None)), (slice(None), rows_of(t))
        arrays = [(dy_in, dy_ref, by_rows), (at_in, at_ref, by_columns), (dyt_in, dyt_ref, by_columns)]
        if last:
            arrays.append((a_in, a_ref, by_rows))
        return [pltpu.make_async_copy(src.at[at], dst.at[at], loads.at[k, t]) for k, (src, dst, at) in enumerate(arrays)]

    def fetch(t, slot):
        return pltpu.make_async_copy(h_ref.at[rows_of(t), :], h.at[slot], h_sem.at[slot])

    def hand_on(t):
        by_rows, by_columns = (rows_of(t), slice(None)), (slice(None), rows_of(t))
        return [
            pltpu.make_async_copy(dy_ref.at[by_rows], dh_ref.at[by_rows], out_sem.at[0, t]),
            pltpu.make_async_copy(dyt_ref.at[by_columns], dht_ref.at[by_columns], out_sem.at[1, t]),
        ]

    def step(t, ends=False):
        rows = rows_of(t)
        if last:
            a = a_ref[rows, :]
            gate, up = dot(a, wg), dot(a, wu)
        else:
            gate, up = gate_ref[rows, :], up_ref[rows, :]
        dy = dy_ref[rows, :]
        dhid = dot_t(dy, wd).astype(BF16).astype(F32)
        sig = jax.nn.sigmoid(gate)
        silu = gate * sig
        hid = (silu * up).astype(BF16)
        dup = (dhid * silu).astype(BF16)
        dgate = (dhid * up * (sig + silu * (1 - sig))).astype(BF16)
        at, dyt = at_ref[:, rows], dyt_ref[:, rows]
        dw[...] += dot(dyt, hid)
        uw[...] += dot(at, dup)
        gw[...] += dot(at, dgate)
        if last:
            da_t = dot_t(dgate, wg) + dot_t(dup, wu)
            if not ends:
                da[rows, :] = jnp.where(i == 0, da_t, da[rows, :] + da_t)
            else:
                wide = h[t % 2].astype(F32)
                scale = scale_of(wide)
                back = (da[rows, :] + da_t).astype(BF16).astype(F32)
                coefficient = jnp.sum(back * wide, -1, keepdims=True) * (scale * scale * scale) * (1.0 / wide.shape[1])
                through = (back * scale - wide * coefficient).astype(BF16)
                dh = (dy.astype(F32) + through.astype(F32)).astype(BF16)
                dy_ref[rows, :] = dh
                dyt_ref[:, rows] = dh.T

    def steps(start, stop):
        def some(n, carry):
            @pl.when(i == 0)
            def _():
                for k in range(unroll):
                    for copy in load(n * unroll + k):
                        copy.wait()

            for k in range(unroll):
                step(n * unroll + k)
            return carry

        def some_last(t, carry):
            fetch(t, t % 2).wait()

            @pl.when(t + 1 < tokens // tile)
            def _():
                fetch(t + 1, (t + 1) % 2).start()

            @pl.when(t > 0)
            def _():
                for copy in hand_on(t - 1):
                    copy.start()

            step(t, ends=True)
            return carry

        if last:

            @pl.when(i < chunks - 1)
            def _():
                lax.fori_loop(start // unroll, stop // unroll, some, 0)

            @pl.when(i == chunks - 1)
            def _():
                if start == 0:
                    fetch(0, 0).start()
                lax.fori_loop(start, stop, some_last, 0)

        else:
            lax.fori_loop(start // unroll, stop // unroll, some, 0)

    for total in (gw, uw, dw):
        total[...] = jnp.zeros_like(total)

    def own(number):
        return for_pair(pair if last else pair.at[number % 3], number)

    @pl.when(i == 0)
    def _():
        for t in range(tokens // tile):
            for copy in load(t):
                copy.start()
        meet((right, left))
        if not last:
            for_pair(pair_in, chunks).start()
            for b in range(3):
                for_down_2(down_in, 0, b).start()
            gg[1] = gg_in[...]
            gu[1] = gu_in[...]
            gd[1] = gd_in[...]

    @pl.when(i > 0)
    def _():
        own(i - 1).start()

    if last:
        half = tokens // tile // 2
        steps(0, half)

        @pl.when(i > 0)
        def _():
            own(i - 1).middle()

    @pl.when(i == 4)
    def _():
        for_down_1().start()

    if not last:

        @pl.when(i == 1)
        def _():
            for_pair(pair_in, chunks).middle()

        @pl.when(i > 1)
        def _():
            own(i - 2).middle()

        @pl.when(i == 2)
        def _():
            for_pair(pair_in, chunks).finish(put_pair((1,), chunks - 1))
            for b in range(3):
                for_down_2(down_in, 0, b).middle()

        @pl.when(i > 2)
        def _():
            own(i - 3).finish(put_pair(layer, i - 3))

        @pl.when(i == 4)
        def _():
            for b in range(3):
                for_down_2(down_in, 0, b).finish(put_down_2(1, b))

    @pl.when(i == (5 if last else 6))
    def _():
        for_down_1().middle()

    if last:

        @pl.when(i == 6)
        def _():
            for_down_1().finish(put_down_1)

        steps(half, 2 * half)

        @pl.when(i > 0)
        def _():
            own(i - 1).finish(put_pair(layer, i - 1))

    else:
        steps(0, tokens // tile)

    at = () if last else (i % 3,)
    pair[(*at, 0)] = gw[...].astype(BF16)
    pair[(*at, 1)] = uw[...].astype(BF16)
    down[pl.ds(pl.multiple_of(c * CHUNK, CHUNK), CHUNK), :] = dw[...].astype(BF16).T

    @pl.when(i == chunks - 1)
    def _():
        if last:
            for copy in hand_on(tokens // tile - 1):
                copy.start()
            for t in range(tokens // tile):
                for copy in hand_on(t):
                    copy.wait()
        else:
            rest = [(for_down_2(down, 1, b), put_down_2(0, b)) for b in range(3)]
            jobs = [own(chunks - 3 + n) for n in range(3)]
            for job in (jobs[2], *(job for job, _ in rest)):
                job.start()
            jobs[1].middle()
            jobs[0].finish(put_pair(layer, chunks - 3))
            for job in (jobs[2], *(job for job, _ in rest)):
                job.middle()
            jobs[1].finish(put_pair(layer, chunks - 2))
            for_down_1().finish(put_down_1)
            for job, put in ((jobs[2], put_pair(layer, chunks - 1)), *rest):
                job.finish(put)


def backward(source, at, dy, dyt, w, layer, h=None, before=None, group=4, tile=512, unroll=1):
    tokens, d = dy.shape
    layers, _, ff = w[0].shape
    last = h is not None
    chunks = ff // CHUNK
    by_columns = pl.BlockSpec((None, d, CHUNK), lambda i: (layer, 0, of(chunks)(i)))
    by_rows = pl.BlockSpec((None, CHUNK, d), lambda i: (layer, of(chunks)(i), 0))
    shapes = [(d // group, ff), (d // group, ff), (ff // group, d), (2, d, CHUNK), (ff, d)]
    dma = pltpu.SemaphoreType.DMA
    slots = chunks - 1 if last else chunks + 1
    part, short = d // group // 2, 2 * CHUNK - ff // group
    scratch = [pltpu.VMEM((d, tokens), BF16), pltpu.VMEM((tokens, d), BF16), pltpu.VMEM((d, tokens), BF16), dma((4, tokens // tile))]
    scratch += [pltpu.VMEM((d, CHUNK), F32)] * 3
    scratch += [pltpu.VMEM((slots, 2, 2, part, CHUNK), BF16), pltpu.VMEM((slots, 2, 2, 2, part, CHUNK), BF16), dma((slots, 6)), dma((slots, 6))]
    scratch += [pltpu.VMEM((2, CHUNK // 2, d), BF16), pltpu.VMEM((2, 2, CHUNK // 2, d), BF16), dma((7, 6)), dma((7, 6))]
    if last:
        out_shape = [jax.ShapeDtypeStruct(s, BF16) for s in ((tokens, d), (d, tokens), *shapes)]
        out_specs = [ANY, ANY] + [whole(s) for s in shapes]
        args = (source, at, dy, dyt, *w, h)
        in_specs = [ANY] * 4 + [by_columns, by_columns, by_rows, ANY]
        scratch = [pltpu.VMEM((tokens, d), BF16)] + scratch + [pltpu.VMEM((tokens, d), F32)]
        scratch += [pltpu.VMEM((2, tile, d), BF16), dma((2,)), dma((2, tokens // tile))]
    else:
        by_chunk = pl.BlockSpec((None, tokens, CHUNK), lambda i: (of(chunks)(i), 0, 0))
        args = (*source, at, dy, dyt, w[2], *before)
        in_specs = [by_chunk, by_chunk] + [ANY] * 3 + [by_rows] + [whole(s) for s in shapes]
        shapes = [(layers, *s) for s in shapes[:3]]
        out_shape = [jax.ShapeDtypeStruct(s, BF16) for s in shapes]
        out_specs = [whole(s) for s in shapes]
        scratch = [pltpu.VMEM((3, 2, d, CHUNK), BF16), pltpu.VMEM((ff, d), BF16)] + scratch
        scratch += [pltpu.VMEM((2, 3, 2, short // 2, d), BF16), pltpu.VMEM((2, 3, 2, 2, short // 2, d), BF16)]
    return pl.pallas_call(
        functools.partial(backward_body, tile, unroll, last),
        grid=(chunks,),
        in_specs=in_specs,
        out_specs=out_specs,
        out_shape=out_shape,
        scratch_shapes=scratch,
        compiler_params=pltpu.CompilerParams(vmem_limit_bytes=VMEM_LIMIT, collective_id=1 if last else 2, has_side_effects=True),
        cost_estimate=pl.CostEstimate(flops=(16 if last else 8) * tokens * d * ff, bytes_accessed=16 * tokens * d, transcendentals=tokens * ff),
        name="backward_last" if last else "backward_first",
    )(*args)


def adamw(w, m, v, g):
    m = 0.9 * m + 0.1 * g
    v = 0.95 * v + 0.05 * g * g
    step = m * lax.rsqrt(v + 1e-8) + 0.1 * w
    return (w - 0.02 * step).astype(BF16), m, v


def update_body(count, *refs):
    g_in, w, m, v, new_w, new_m, new_v, g = (refs[k : k + 3] for k in range(0, 24, 3))
    mine, sums, norm_send, norm_recv, load, send, recv = refs[24:]
    me, right, left, far = ring()
    layers = g[0].shape[0]
    loads = {}

    def fetch(which, k, layer, src, dst, at):
        loads[k, layer, which] = pltpu.make_async_copy(src[k].at[at], dst[k].at[at], load.at[k, layer, which])
        loads[k, layer, which].start()

    parts = [(k, layer) for k in range(3) for layer in range(layers)]
    for k, layer in parts:
        fetch(3, k, layer, g_in, g, layer)
    for k, layer in parts:
        fetch(0, k, layer, w, new_w, (layer, pl.ds(pl.multiple_of(me * g[k].shape[1], 32), g[k].shape[1])))
        fetch(1, k, layer, m, new_m, layer)
        fetch(2, k, layer, v, new_v, layer)
    meet((right, left, far))
    total = jnp.float32(0)
    for k in range(3):
        for layer in range(layers):
            loads[k, layer, 3].wait()

            def add(r, squares):
                part = g[k][layer, pl.ds(pl.multiple_of(r * 16, 16), 16), :].astype(F32)
                return squares + part * part

            total += jnp.sum(lax.fori_loop(0, g[k].shape[1] // 16, add, jnp.zeros((16, g[k].shape[2]), F32)))
    mine[...] = jnp.full(mine.shape, total, F32)
    sums[me] = mine[...]
    tells = [remote(mine, sums.at[me], norm_send.at[n], norm_recv.at[n], to) for n, to in enumerate((right, left, far))]
    for tell in tells:
        tell.start()
    for tell in tells:
        tell.wait()
    squares = sum(sums[n] for n in range(sums.shape[0]))
    factor = jnp.minimum(1.0, 0.5 * lax.rsqrt(squares / count + 1e-30))[0:1, 0:1]

    copies = []
    for k in range(3):
        size, rows = g[k].shape[1], 32
        half = size // 2
        for layer in range(layers):
            for which in range(3):
                loads[k, layer, which].wait()

            def change(r, carry):
                at = (layer, pl.ds(pl.multiple_of(r * rows, rows), rows), slice(None))
                own = (layer, pl.ds(pl.multiple_of(me * size + r * rows, rows), rows), slice(None))
                new = adamw(new_w[k][own].astype(F32), new_m[k][at], new_v[k][at], g[k][at].astype(F32) * factor)
                new_w[k][own], new_m[k][at], new_v[k][at] = new
                return carry

            lax.fori_loop(0, size // rows, change, 0)

            def block(owner, start, length):
                return new_w[k].at[layer, pl.ds(pl.multiple_of(owner * size + start, 32), length), :]

            s, r = send.at[k, layer], recv.at[k, layer]
            direct = [remote(block(me, 0, size), block(me, 0, size), s.at[n], r.at[n], to) for n, to in enumerate((right, left))]
            on = [
                remote(block(left, 0, half), block(left, 0, half), s.at[2], r.at[2], right),
                remote(block(right, half, half), block(right, half, half), s.at[3], r.at[3], left),
            ]
            for copy in direct:
                copy.start()
            copies.append((direct, on))
    for direct, on in copies:
        for first, second in zip(direct, on, strict=True):
            first.wait_recv()
            second.start()
    for direct, on in copies:
        for copy in on:
            copy.wait()
        for copy in direct:
            copy.wait_send()


def update(g, w, m, v):
    count = sum(t.size for t in w)
    layers = w[0].shape[0]
    shapes = [pltpu.VMEM(t.shape, t.dtype) for t in (*w, *m, *v)]
    dma = pltpu.SemaphoreType.DMA
    group = w[0].shape[1] // m[0].shape[1]
    vmem = pl.BlockSpec(memory_space=pltpu.VMEM)
    return pl.pallas_call(
        functools.partial(update_body, count),
        in_specs=[ANY] * 12,
        out_specs=[vmem] * 9,
        out_shape=shapes,
        scratch_shapes=[pltpu.VMEM(t.shape, BF16) for t in m]
        + [pltpu.VMEM((8, 128), F32), pltpu.VMEM((group, 8, 128), F32), dma((3,)), dma((3,))]
        + [dma((3, layers, 4)), dma((3, layers, 4)), dma((3, layers, 4))],
        compiler_params=pltpu.CompilerParams(vmem_limit_bytes=28_000_000, collective_id=3, has_side_effects=True),
        name="update",
    )(*g, *w, *m, *v)


def solution(mesh):
    group = mesh.shape["dp"]

    def step(x, dy, *arrays):
        w, m, v = (arrays[i : i + 3] for i in (0, 3, 6))
        x, dy = x[0], dy[0]
        gate, up, a1t, h1, a2, a2t, dyt = forward(x, dy, *w, 0)
        dh, dht, *before = backward(a2, a2t, dy, dyt, w, 1, h=h1, group=group)
        g = backward((gate, up), a1t, dh, dht, w, 0, before=before, group=group, unroll=4)
        return tuple(update(g, w, m, v))

    sequence, rows = P(("rep", "dp"), None, None), P(None, "dp", None)
    return jax.shard_map(
        step,
        mesh=mesh,
        in_specs=(sequence,) * 2 + (P(),) * 3 + (rows,) * 6,
        out_specs=(P("rep", None, None),) * 3 + (P("rep", "dp", None),) * 6,
        check_vma=False,
    )
```

```python
import functools

import jax
import jax.numpy as jnp
from jax import lax
from jax.experimental import pallas as pl
from jax.experimental.pallas import tpu as pltpu
from jax.sharding import PartitionSpec as P

F32, BF16 = jnp.float32, jnp.bfloat16
VMEM_LIMIT = 66_000_000
CHUNK = 256
MESH = pl.DeviceIdType.MESH
ANY = pl.BlockSpec(memory_space=pl.ANY)


def dot(a, b):
    return jnp.dot(a, b, preferred_element_type=F32)


def dot_t(a, b):
    return lax.dot_general(a, b, (((1,), (1,)), ((), ())), preferred_element_type=F32)


def scale_of(wide):
    return lax.rsqrt(jnp.mean(wide * wide, -1, keepdims=True) + 1e-6)


def whole(shape, at=None):
    if at is None:
        return pl.BlockSpec(shape, lambda *_: (0,) * len(shape), pipeline_mode=pl.Buffered(1))
    return pl.BlockSpec((None, *shape), lambda *_: (at,) + (0,) * len(shape), pipeline_mode=pl.Buffered(1))


def ring():
    n = lax.axis_size("dp")
    me = lax.axis_index("dp")
    return me, (me + 1) % n, (me + n - 1) % n, (me + 2) % n


def meet(others):
    barrier = pltpu.get_barrier_semaphore()
    for other in others:
        pl.semaphore_signal(barrier, inc=1, device_id={"dp": other}, device_id_type=MESH)
    pl.semaphore_wait(barrier, len(others))


def remote(src, dst, send, recv, to):
    return pltpu.make_async_remote_copy(src_ref=src, dst_ref=dst, send_sem=send, recv_sem=recv, device_id={"dp": to}, device_id_type=MESH)


class Scatter:
    def __init__(self, piece, landed, final, send, recv):
        self.piece, self.landed, self.final = piece, landed, final
        self.me, right, left, far = ring()
        self.right, self.left = right, left
        self.routes = (
            lambda: (piece(far, 0), landed.at[0], right),
            lambda: (piece(far, 1), landed.at[1], left),
            lambda: (piece(right, 1), final.at[0, 1], right),
            lambda: (piece(left, 0), final.at[1, 0], left),
            lambda: (landed.at[0], final.at[0, 0], right),
            lambda: (landed.at[1], final.at[1, 1], left),
        )
        self.semaphores = send, recv

    def copy(self, k):
        src, dst, to = self.routes[k]()
        return remote(src, dst, self.semaphores[0].at[k], self.semaphores[1].at[k], to)

    def start(self):
        for k in range(4):
            self.copy(k).start()

    def middle(self):
        for k, own in enumerate((self.piece(self.right, 0), self.piece(self.left, 1))):
            self.copy(k).wait_recv()
            self.landed[k] = (self.landed[k].astype(F32) + own[...].astype(F32)).astype(BF16)
        for k in range(4, 6):
            self.copy(k).start()

    def finish(self, put):
        for k in range(2, 6):
            self.copy(k).wait_recv()
        for half in range(2):
            total = self.piece(self.me, half)[...].astype(F32) + self.final[0, half].astype(F32) + self.final[1, half].astype(F32)
            put(half, total.astype(BF16))
        for k in range(6):
            self.copy(k).wait_send()


def forward_body(x_ref, dy_ref, wg_ref, wu_ref, wd_ref, gate_ref, up_ref, hid_ref, at_ref, h_ref, a2_ref, a2t_ref, dyt_ref, hid):
    x = x_ref[...].astype(F32)
    a = (x * scale_of(x)).astype(BF16)
    for j in range(wg_ref.shape[1] // CHUNK):
        at = slice(j * CHUNK, (j + 1) * CHUNK)
        gate, up = dot(a, wg_ref[:, at]), dot(a, wu_ref[:, at])
        gate_ref[j], up_ref[j] = gate, up
        hid[:, at] = hid_ref[j] = (gate * jax.nn.sigmoid(gate) * up).astype(BF16)
    at_ref[...] = a.T
    dyt_ref[...] = dy_ref[...].T
    h = (x + dot(hid[...], wd_ref[...]).astype(BF16).astype(F32)).astype(BF16)
    h_ref[...] = h
    wide = h.astype(F32)
    a2 = (wide * scale_of(wide)).astype(BF16)
    a2_ref[...] = a2
    a2t_ref[...] = a2.T


def forward(x, dy, wg, wu, wd, layer, tile=512):
    tokens, d = x.shape
    ff = wg.shape[2]
    chunks = ff // CHUNK
    rows = pl.BlockSpec((tile, d), lambda i: (i, 0))
    columns = pl.BlockSpec((d, tile), lambda i: (0, i))
    kept = pl.BlockSpec((chunks, tile, CHUNK), lambda i: (0, i, 0))
    flat, turned = jax.ShapeDtypeStruct((tokens, d), BF16), jax.ShapeDtypeStruct((d, tokens), BF16)
    by_chunk = (chunks, tokens, CHUNK)
    return pl.pallas_call(
        forward_body,
        grid=(tokens // tile,),
        in_specs=[rows, rows, whole((d, ff), layer), whole((d, ff), layer), whole((ff, d), layer)],
        out_specs=[kept, kept, kept, columns, rows, rows, columns, columns],
        out_shape=[*(jax.ShapeDtypeStruct(by_chunk, t) for t in (F32, F32, BF16)), turned, flat, flat, turned, turned],
        scratch_shapes=[pltpu.VMEM((tile, ff), BF16)],
        compiler_params=pltpu.CompilerParams(vmem_limit_bytes=VMEM_LIMIT),
        cost_estimate=pl.CostEstimate(flops=6 * tokens * d * ff, bytes_accessed=16 * tokens * d, transcendentals=tokens * ff),
        name="forward",
    )(x, dy, wg, wu, wd)


def of(n):
    return lambda i: (2 * i) % n


def aligned(start, length, unit):
    return pl.ds(pl.multiple_of(start, unit), length)


def pair_job(ref, slot, landed, final, send, recv):
    part = landed.shape[-2]
    return Scatter(lambda owner, half: ref.at[:, aligned((2 * owner + half) * part, part, 32), :], landed.at[slot], final.at[slot], send.at[slot], recv.at[slot])


def put_pair(gg, gu, layer, chunk):
    def put(half, value):
        part = value.shape[1]
        at = (*layer, slice(half * part, (half + 1) * part), aligned(chunk * CHUNK, CHUNK, CHUNK))
        gg[at], gu[at] = value[0], value[1]

    return put


def down_job(ref, start, slot, landed, final, send, recv):
    part = landed.shape[-2]
    return Scatter(lambda owner, half: ref.at[aligned(start(owner) + half * part, part, 16), :], landed.at[slot], final.at[slot], send.at[slot], recv.at[slot])


def put_down(gd, layer, start):
    def put(half, value):
        part = value.shape[0]
        gd[(*layer, aligned(start + half * part, part, 16), slice(None))] = value

    return put


def left_over(owner, b, share):
    short = 2 * CHUNK - share
    return b * short + (1 - (owner - b + 3) // 4) * CHUNK


def gradients_of(gate, up, dhid):
    sig = jax.nn.sigmoid(gate)
    silu = gate * sig
    return (silu * up).astype(BF16), (dhid * up * (sig + silu * (1 - sig))).astype(BF16), (dhid * silu).astype(BF16)


def last_body(tile, unroll, *refs):
    a_in, at_in, dy_in, dyt_in, wg_ref, wu_ref, wd_ref, h_ref, dh_ref, dht_ref, gg, gu, gd, pair, down, a_ref, at_ref, dy_ref, dyt_ref, loads, gw, uw, dw, *rest = refs
    (*pairs, landed1, final1, send1, recv1, da, h, h_sem, out_sem) = rest
    tokens, d = dy_ref.shape
    share = gd.shape[0]
    i, chunks = pl.program_id(0), pl.num_programs(0)
    order = of(chunks)
    me, right, left, far = ring()
    n_tiles = tokens // tile
    wg, wu, wd = wg_ref[...], wu_ref[...], wd_ref[...]
    wgu = jnp.concatenate([wg, wu], 1)

    def own(number):
        return pair_job(pair, number, *pairs)

    def evens():
        return down_job(down, lambda owner: owner * 2 * CHUNK, 0, landed1, final1, send1, recv1)

    def rows_of(t):
        return aligned(t * tile, tile, tile)

    def load(t):
        by_rows, by_columns = (rows_of(t), slice(None)), (slice(None), rows_of(t))
        arrays = (dy_in, dy_ref, by_rows), (a_in, a_ref, by_rows), (at_in, at_ref, by_columns), (dyt_in, dyt_ref, by_columns)
        return [pltpu.make_async_copy(src.at[at], dst.at[at], loads.at[k, t]) for k, (src, dst, at) in enumerate(arrays)]

    def fetch(t, slot):
        return pltpu.make_async_copy(h_ref.at[rows_of(t), :], h.at[slot], h_sem.at[slot])

    def hand_on(t):
        by_rows, by_columns = (rows_of(t), slice(None)), (slice(None), rows_of(t))
        return [
            pltpu.make_async_copy(dy_ref.at[by_rows], dh_ref.at[by_rows], out_sem.at[0, t]),
            pltpu.make_async_copy(dyt_ref.at[by_columns], dht_ref.at[by_columns], out_sem.at[1, t]),
        ]

    def step(t, ends=False):
        rows = rows_of(t)
        a, dy = a_ref[rows, :], dy_ref[rows, :]
        hid, dgate, dup = gradients_of(dot(a, wg), dot(a, wu), dot_t(dy, wd).astype(BF16).astype(F32))
        at, dyt = at_ref[:, rows], dyt_ref[:, rows]
        dw[...] += dot(dyt, hid)
        uw[...] += dot(at, dup)
        gw[...] += dot(at, dgate)
        da_t = dot_t(jnp.concatenate([dgate, dup], 1), wgu)
        if not ends:
            da[rows, :] = jnp.where(i == 0, da_t, da[rows, :] + da_t)
        else:
            wide = h[t % 2].astype(F32)
            scale = scale_of(wide)
            back = (da[rows, :] + da_t).astype(BF16).astype(F32)
            coefficient = jnp.sum(back * wide, -1, keepdims=True) * (scale * scale * scale) * (1.0 / wide.shape[1])
            through = (back * scale - wide * coefficient).astype(BF16)
            dh = (dy.astype(F32) + through.astype(F32)).astype(BF16)
            dy_ref[rows, :] = dh
            dyt_ref[:, rows] = dh.T

    def steps(start, stop):
        def some(m, carry):
            @pl.when(i == 0)
            def _():
                for k in range(unroll):
                    for copy in load(m * unroll + k):
                        copy.wait()

            for k in range(unroll):
                step(m * unroll + k)
            return carry

        def some_last(t, carry):
            fetch(t, t % 2).wait()

            @pl.when(t + 1 < n_tiles)
            def _():
                fetch(t + 1, (t + 1) % 2).start()

            @pl.when(t > 0)
            def _():
                for copy in hand_on(t - 1):
                    copy.start()

            step(t, ends=True)
            return carry

        @pl.when(i < chunks - 1)
        def _():
            lax.fori_loop(start // unroll, stop // unroll, some, 0)

        @pl.when(i == chunks - 1)
        def _():
            if start == 0:
                fetch(0, 0).start()
            lax.fori_loop(start, stop, some_last, 0)

    for total in (gw, uw, dw):
        total[...] = jnp.zeros_like(total)

    @pl.when(i == 0)
    def _():
        for t in range(n_tiles):
            for copy in load(t):
                copy.start()
        meet((right, left))

    @pl.when(i > 0)
    def _():
        own(i - 1).start()

    steps(0, n_tiles // 2)

    @pl.when(i > 0)
    def _():
        own(i - 1).middle()

    @pl.when(i == 4)
    def _():
        evens().start()

    @pl.when(i == 5)
    def _():
        evens().middle()

    @pl.when(i == 6)
    def _():
        evens().finish(put_down(gd, (), me * (2 * CHUNK - share)))

    steps(n_tiles // 2, n_tiles)

    @pl.when(i > 0)
    def _():
        own(i - 1).finish(put_pair(gg, gu, (), order(i - 1)))

    pair[0] = gw[...].astype(BF16)
    pair[1] = uw[...].astype(BF16)
    down[aligned(order(i) * CHUNK, CHUNK, CHUNK), :] = dw[...].astype(BF16).T

    @pl.when(i == chunks - 1)
    def _():
        for copy in hand_on(n_tiles - 1):
            copy.start()
        for t in range(n_tiles):
            for copy in hand_on(t):
                copy.wait()


def first_body(tile, unroll, *refs):
    gate_in, up_in, hid_ref, at_in, dy_in, dyt_in, wd_ref, gg_in, gu_in, gd_in, pair_in, down_hbm, gg, gu, gd, pair, down, down_in, kept, kept_sem, g_sem, at_ref, dy_ref, dyt_ref, loads, gw, uw, by, *rest = refs
    pairs, downs, leftovers = rest[:4], rest[4:8], rest[8:]
    tokens, d = dy_ref.shape
    share = gd.shape[-2]
    i, chunks = pl.program_id(0), down.shape[0] // CHUNK
    n = i - chunks
    me, right, left, far = ring()
    n_tiles = tokens // tile
    runs = downs[0].shape[0]
    run = share // runs

    def held(row):
        return row // (2 * CHUNK) * CHUNK + row % CHUNK

    def odd_chunks():
        return [
            pltpu.make_async_copy(down_hbm.at[(2 * b + 1) * CHUNK : (2 * b + 2) * CHUNK, :], down_in.at[b * CHUNK : (b + 1) * CHUNK, :], g_sem.at[3 + b])
            for b in range(chunks // 2)
        ]

    def before():
        jobs = [(pair_job(pair_in, chunks, *pairs), put_pair(gg, gu, (1,), of(chunks)(chunks - 1)))]
        for b in range(3):
            start = functools.partial(left_over, b=b, share=share)
            jobs.append((down_job(down_in, lambda owner, start=start: held(owner * share + start(owner)), b, *leftovers), put_down(gd, (1,), start(me))))
        return jobs

    def own(number):
        return pair_job(pair.at[number % 3], number, *pairs), put_pair(gg, gu, (0,), number)

    def rows_job(number):
        return down_job(down, lambda owner: owner * share + number * run, number, *downs), put_down(gd, (0,), number * run)

    def rows_of(t):
        return aligned(t * tile, tile, tile)

    def load(k, t):
        by_rows, by_columns = (rows_of(t), slice(None)), (slice(None), rows_of(t))
        src, dst, at = ((dyt_in, dyt_ref, by_columns), (dy_in, dy_ref, by_rows), (at_in, at_ref, by_columns))[k]
        return pltpu.make_async_copy(src.at[at], dst.at[at], loads.at[k, t])

    def keep(number):
        return [pltpu.make_async_copy(src.at[number], kept.at[number % 2, k], kept_sem.at[number % 2, k]) for k, src in enumerate((gate_in, up_in))]

    def g_before():
        return [pltpu.make_async_copy(src, dst.at[1], g_sem.at[k]) for k, (src, dst) in enumerate(((gg_in, gg), (gu_in, gu), (gd_in, gd)))]

    @pl.when(i == 0)
    def _():
        for copy in odd_chunks() + [load(0, t) for t in range(n_tiles)] + g_before() + [load(k, t) for t in range(n_tiles) for k in (1, 2)] + keep(0):
            copy.start()
        meet((right, left))
        for copy in odd_chunks():
            copy.wait()
        for job, _ in before():
            job.start()

    @pl.when(i == 4)
    def _():
        before()[0][0].middle()

    @pl.when(i == 6)
    def _():
        for copy in g_before():
            copy.wait()
        jobs = before()
        for job, _ in jobs[1:]:
            job.middle()
        jobs[0][0].finish(jobs[0][1])

    @pl.when(i == chunks + 1)
    def _():
        for job, put in before()[1:]:
            job.finish(put)

    @pl.when(n < 0)
    def _():
        gw[...] = jnp.zeros_like(gw)

        def some(t, carry):
            @pl.when(i == 0)
            def _():
                for k in range(unroll):
                    load(0, t * unroll + k).wait()

            rows = pl.ds(pl.multiple_of(t * tile * unroll, tile * unroll), tile * unroll)
            gw[...] += dot(dyt_ref[:, rows], hid_ref[rows, :])
            return carry

        lax.fori_loop(0, n_tiles // unroll, some, 0)
        down[aligned(i * CHUNK, CHUNK, CHUNK), :] = gw[...].astype(BF16).T

    @pl.when(n >= 1)
    def _():
        own(n - 1)[0].start()

    for b in range(2):

        @pl.when(n == b)
        def _():
            rows_job(b)[0].start()

    @pl.when(n >= 2)
    def _():
        own(n - 2)[0].middle()

    for b in range(2):

        @pl.when(n == b + 2)
        def _():
            rows_job(b)[0].middle()

    @pl.when(n >= 3)
    def _():
        job, put = own(n - 3)
        job.finish(put)

    for b in range(2):

        @pl.when(n == b + 4)
        def _():
            job, put = rows_job(b)
            job.finish(put)

    @pl.when(n >= 0)
    def _():
        @pl.when(n + 1 < chunks)
        def _():
            for copy in keep(n + 1):
                copy.start()

        gw[...] = jnp.zeros_like(gw)
        uw[...] = jnp.zeros_like(uw)
        wd = wd_ref[...]
        for copy in keep(n):
            copy.wait()
        slot = n % 2

        def some(m, carry):
            @pl.when(n == 0)
            def _():
                for k in range(unroll):
                    for which in (1, 2):
                        load(which, m * unroll + k).wait()

            for k in range(unroll):
                rows = rows_of(m * unroll + k)
                dhid = dot_t(dy_ref[rows, :], wd).astype(BF16).astype(F32)
                _, dgate, dup = gradients_of(kept[slot, 0, rows, :], kept[slot, 1, rows, :], dhid)
                by[0, k * tile : (k + 1) * tile, :] = dgate
                by[1, k * tile : (k + 1) * tile, :] = dup
            at = at_ref[:, aligned(m * unroll * tile, unroll * tile, unroll * tile)]
            gw[...] += dot(at, by[0])
            uw[...] += dot(at, by[1])
            return carry

        lax.fori_loop(0, n_tiles // unroll, some, 0)
        pair[n % 3, 0] = gw[...].astype(BF16)
        pair[n % 3, 1] = uw[...].astype(BF16)

    @pl.when(n == chunks - 1)
    def _():
        ends = [own(chunks - 3 + k) for k in range(3)]
        ends[2][0].start()
        ends[1][0].middle()
        ends[0][0].finish(ends[0][1])
        ends[2][0].middle()
        for job, put in ends[1:]:
            job.finish(put)


def scatter_scratch(jobs, *half):
    dma = pltpu.SemaphoreType.DMA
    return [pltpu.VMEM((jobs, 2, *half), BF16), pltpu.VMEM((jobs, 2, 2, *half), BF16), dma((jobs, 6)), dma((jobs, 6))]


def shares(w, group):
    _, d, ff = w[0].shape
    return [(d // group, ff), (d // group, ff), (ff // group, d)]


def backward_last(a, at, dy, dyt, w, layer, h, group, tile=512, unroll=1):
    tokens, d = dy.shape
    _, _, ff = w[0].shape
    chunks = ff // CHUNK
    by_columns = pl.BlockSpec((None, d, CHUNK), lambda i: (layer, 0, of(chunks)(i)))
    by_rows = pl.BlockSpec((None, CHUNK, d), lambda i: (layer, of(chunks)(i), 0))
    shapes = shares(w, group) + [(2, d, CHUNK), (ff, d)]
    dma = pltpu.SemaphoreType.DMA
    scratch = [pltpu.VMEM((tokens, d), BF16), pltpu.VMEM((d, tokens), BF16)] * 2 + [dma((4, tokens // tile))]
    scratch += [pltpu.VMEM((d, CHUNK), F32)] * 3
    scratch += scatter_scratch(chunks - 1, 2, d // group // 2, CHUNK) + scatter_scratch(1, CHUNK // 2, d)
    scratch += [pltpu.VMEM((tokens, d), F32), pltpu.VMEM((2, tile, d), BF16), dma((2,)), dma((2, tokens // tile))]
    return pl.pallas_call(
        functools.partial(last_body, tile, unroll),
        grid=(chunks,),
        in_specs=[ANY] * 4 + [by_columns, by_columns, by_rows, ANY],
        out_specs=[ANY, ANY] + [whole(s) for s in shapes],
        out_shape=[jax.ShapeDtypeStruct(s, BF16) for s in ((tokens, d), (d, tokens), *shapes)],
        scratch_shapes=scratch,
        compiler_params=pltpu.CompilerParams(vmem_limit_bytes=VMEM_LIMIT, collective_id=1, has_side_effects=True),
        cost_estimate=pl.CostEstimate(flops=16 * tokens * d * ff, bytes_accessed=16 * tokens * d, transcendentals=tokens * ff),
        name="backward_last",
    )(a, at, dy, dyt, *w, h)


def backward_first(gate, up, hid, at, dy, dyt, w, layer, before, group, tile=512, unroll=4):
    tokens, d = dy.shape
    layers, _, ff = w[0].shape
    chunks = ff // CHUNK
    by_chunk = pl.BlockSpec((None, tokens, CHUNK), lambda i: (jnp.minimum(i, chunks - 1), 0, 0))
    by_rows = pl.BlockSpec((None, CHUNK, d), lambda i: (layer, jnp.maximum(i - chunks, 0), 0))
    shapes = [(layers, *s) for s in shares(w, group)]
    dma = pltpu.SemaphoreType.DMA
    short = 2 * CHUNK - ff // group
    scratch = [pltpu.VMEM((3, 2, d, CHUNK), BF16), pltpu.VMEM((ff, d), BF16), pltpu.VMEM((chunks // 2 * CHUNK, d), BF16)]
    scratch += [pltpu.VMEM((2, 2, tokens, CHUNK), F32), dma((2, 2)), dma((3 + chunks // 2,))]
    scratch += [pltpu.VMEM((d, tokens), BF16), pltpu.VMEM((tokens, d), BF16), pltpu.VMEM((d, tokens), BF16), dma((3, tokens // tile))]
    scratch += [pltpu.VMEM((d, CHUNK), F32)] * 2 + [pltpu.VMEM((2, unroll * tile, CHUNK), BF16)]
    scratch += scatter_scratch(chunks + 1, 2, d // group // 2, CHUNK) + scatter_scratch(2, ff // group // 4, d) + scatter_scratch(3, short // 2, d)
    return pl.pallas_call(
        functools.partial(first_body, tile, unroll),
        grid=(2 * chunks,),
        in_specs=[ANY, ANY, by_chunk] + [ANY] * 3 + [by_rows] + [ANY] * 3 + [whole((2, d, CHUNK)), ANY],
        out_specs=[whole(s) for s in shapes],
        out_shape=[jax.ShapeDtypeStruct(s, BF16) for s in shapes],
        scratch_shapes=scratch,
        compiler_params=pltpu.CompilerParams(vmem_limit_bytes=VMEM_LIMIT, collective_id=2, has_side_effects=True),
        cost_estimate=pl.CostEstimate(flops=8 * tokens * d * ff, bytes_accessed=16 * tokens * d, transcendentals=tokens * ff),
        name="backward_first",
    )(gate, up, hid, at, dy, dyt, w[2], *before)


def adamw(w, m, v, g):
    m = 0.9 * m + 0.1 * g
    v = 0.95 * v + 0.05 * g * g
    step = m * lax.rsqrt(v + 1e-8) + 0.1 * w
    return (w - 0.02 * step).astype(BF16), m, v


def update_body(count, *refs):
    g_in, w, m, v, new_w, new_m, new_v, g = (refs[k : k + 3] for k in range(0, 24, 3))
    mine, sums, norm_send, norm_recv, load, send, recv = refs[24:]
    me, right, left, far = ring()
    layers = g[0].shape[0]
    loads = {}

    def fetch(which, k, layer, src, dst, at):
        loads[k, layer, which] = pltpu.make_async_copy(src[k].at[at], dst[k].at[at], load.at[k, layer, which])
        loads[k, layer, which].start()

    parts = [(k, layer) for k in range(3) for layer in range(layers)]
    for k, layer in parts:
        fetch(3, k, layer, g_in, g, layer)
    for k, layer in parts:
        fetch(0, k, layer, w, new_w, (layer, pl.ds(pl.multiple_of(me * g[k].shape[1], 32), g[k].shape[1])))
        fetch(1, k, layer, m, new_m, layer)
        fetch(2, k, layer, v, new_v, layer)
    meet((right, left, far))
    total = jnp.float32(0)
    for k in range(3):
        for layer in range(layers):
            loads[k, layer, 3].wait()

            def add(r, squares):
                part = g[k][layer, pl.ds(pl.multiple_of(r * 16, 16), 16), :].astype(F32)
                return squares + part * part

            total += jnp.sum(lax.fori_loop(0, g[k].shape[1] // 16, add, jnp.zeros((16, g[k].shape[2]), F32)))
    mine[...] = jnp.full(mine.shape, total, F32)
    sums[me] = mine[...]
    tells = [remote(mine, sums.at[me], norm_send.at[n], norm_recv.at[n], to) for n, to in enumerate((right, left, far))]
    for tell in tells:
        tell.start()
    for tell in tells:
        tell.wait()
    squares = sum(sums[n] for n in range(sums.shape[0]))
    factor = jnp.minimum(1.0, 0.5 * lax.rsqrt(squares / count + 1e-30))[0:1, 0:1]

    copies = []
    for k in range(3):
        size, rows = g[k].shape[1], 32
        half = size // 2
        for layer in range(layers):
            for which in range(3):
                loads[k, layer, which].wait()

            def change(r, carry):
                at = (layer, pl.ds(pl.multiple_of(r * rows, rows), rows), slice(None))
                own = (layer, pl.ds(pl.multiple_of(me * size + r * rows, rows), rows), slice(None))
                new = adamw(new_w[k][own].astype(F32), new_m[k][at], new_v[k][at], g[k][at].astype(F32) * factor)
                new_w[k][own], new_m[k][at], new_v[k][at] = new
                return carry

            lax.fori_loop(0, size // rows, change, 0)

            def block(owner, start, length):
                return new_w[k].at[layer, pl.ds(pl.multiple_of(owner * size + start, 32), length), :]

            s, r = send.at[k, layer], recv.at[k, layer]
            direct = [remote(block(me, 0, size), block(me, 0, size), s.at[n], r.at[n], to) for n, to in enumerate((right, left))]
            on = [
                remote(block(left, 0, half), block(left, 0, half), s.at[2], r.at[2], right),
                remote(block(right, half, half), block(right, half, half), s.at[3], r.at[3], left),
            ]
            for copy in direct:
                copy.start()
            copies.append((direct, on))
    for direct, on in copies:
        for first, second in zip(direct, on, strict=True):
            first.wait_recv()
            second.start()
    for direct, on in copies:
        for copy in on:
            copy.wait()
        for copy in direct:
            copy.wait_send()


def update(g, w, m, v):
    count = sum(t.size for t in w)
    layers = w[0].shape[0]
    shapes = [pltpu.VMEM(t.shape, t.dtype) for t in (*w, *m, *v)]
    dma = pltpu.SemaphoreType.DMA
    group = w[0].shape[1] // m[0].shape[1]
    vmem = pl.BlockSpec(memory_space=pltpu.VMEM)
    return pl.pallas_call(
        functools.partial(update_body, count),
        in_specs=[ANY] * 12,
        out_specs=[vmem] * 9,
        out_shape=shapes,
        scratch_shapes=[pltpu.VMEM(t.shape, BF16) for t in m]
        + [pltpu.VMEM((8, 128), F32), pltpu.VMEM((group, 8, 128), F32), dma((3,)), dma((3,))]
        + [dma((3, layers, 4)), dma((3, layers, 4)), dma((3, layers, 4))],
        compiler_params=pltpu.CompilerParams(vmem_limit_bytes=28_000_000, collective_id=3, has_side_effects=True),
        name="update",
    )(*g, *w, *m, *v)


def deliver_body(*refs):
    copies = [pltpu.make_async_copy(refs[k], refs[9 + k], refs[18].at[k]) for k in range(9)]
    for copy in copies:
        copy.start()
    for copy in copies:
        copy.wait()


def deliver(arrays):
    arrays = [pltpu.with_memory_space_constraint(t, pltpu.VMEM) for t in arrays]
    return pl.pallas_call(
        deliver_body,
        in_specs=[pl.BlockSpec(memory_space=pltpu.VMEM)] * 9,
        out_specs=[ANY] * 9,
        out_shape=[jax.ShapeDtypeStruct(t.shape, t.dtype) for t in arrays],
        scratch_shapes=[pltpu.SemaphoreType.DMA((9,))],
        compiler_params=pltpu.CompilerParams(vmem_limit_bytes=28_000_000),
        name="deliver",
    )(*arrays)


def solution(mesh):
    group = mesh.shape["dp"]

    def step(x, dy, *arrays):
        w, m, v = (arrays[i : i + 3] for i in (0, 3, 6))
        x, dy = x[0], dy[0]
        gate, up, hid, a1t, h1, a2, a2t, dyt = forward(x, dy, *w, 0)
        dh, dht, *before = backward_last(a2, a2t, dy, dyt, w, 1, h1, group)
        g = backward_first(gate, up, hid, a1t, dh, dht, w, 0, before, group)
        return tuple(deliver(update(g, w, m, v)))

    sequence, rows = P(("rep", "dp"), None, None), P(None, "dp", None)
    return jax.shard_map(
        step,
        mesh=mesh,
        in_specs=(sequence,) * 2 + (P(),) * 3 + (rows,) * 6,
        out_specs=(P("rep", None, None),) * 3 + (P("rep", "dp", None),) * 6,
        check_vma=False,
    )
```

```python
import functools

import jax
import jax.numpy as jnp
from jax import lax
from jax.experimental import pallas as pl
from jax.experimental.pallas import tpu as pltpu
from jax.sharding import PartitionSpec as P

F32, BF16 = jnp.float32, jnp.bfloat16
VMEM_LIMIT = 66_000_000
CHUNK = 256
MESH = pl.DeviceIdType.MESH
ANY = pl.BlockSpec(memory_space=pl.ANY)


def dot(a, b):
    return jnp.dot(a, b, preferred_element_type=F32)


def dot_t(a, b):
    return lax.dot_general(a, b, (((1,), (1,)), ((), ())), preferred_element_type=F32)


def scale_of(wide):
    return lax.rsqrt(jnp.mean(wide * wide, -1, keepdims=True) + 1e-6)


def whole(shape, at=None):
    if at is None:
        return pl.BlockSpec(shape, lambda *_: (0,) * len(shape), pipeline_mode=pl.Buffered(1))
    return pl.BlockSpec((None, *shape), lambda *_: (at,) + (0,) * len(shape), pipeline_mode=pl.Buffered(1))


def ring():
    n = lax.axis_size("dp")
    me = lax.axis_index("dp")
    return me, (me + 1) % n, (me + n - 1) % n, (me + 2) % n


def meet(others):
    barrier = pltpu.get_barrier_semaphore()
    for other in others:
        pl.semaphore_signal(barrier, inc=1, device_id={"dp": other}, device_id_type=MESH)
    pl.semaphore_wait(barrier, len(others))


def remote(src, dst, send, recv, to):
    return pltpu.make_async_remote_copy(src_ref=src, dst_ref=dst, send_sem=send, recv_sem=recv, device_id={"dp": to}, device_id_type=MESH)


class Scatter:
    def __init__(self, piece, landed, final, send, recv):
        self.piece, self.landed, self.final = piece, landed, final
        self.me, right, left, far = ring()
        self.right, self.left = right, left
        self.routes = (
            lambda: (piece(far, 0), landed.at[0], right),
            lambda: (piece(far, 1), landed.at[1], left),
            lambda: (piece(right, 1), final.at[0, 1], right),
            lambda: (piece(left, 0), final.at[1, 0], left),
            lambda: (landed.at[0], final.at[0, 0], right),
            lambda: (landed.at[1], final.at[1, 1], left),
        )
        self.semaphores = send, recv

    def copy(self, k):
        src, dst, to = self.routes[k]()
        return remote(src, dst, self.semaphores[0].at[k], self.semaphores[1].at[k], to)

    def start(self):
        for k in range(4):
            self.copy(k).start()

    def middle(self):
        for k, own in enumerate((self.piece(self.right, 0), self.piece(self.left, 1))):
            self.copy(k).wait_recv()
            self.landed[k] = (self.landed[k].astype(F32) + own[...].astype(F32)).astype(BF16)
        for k in range(4, 6):
            self.copy(k).start()

    def finish(self, put):
        for k in range(2, 6):
            self.copy(k).wait_recv()
        for half in range(2):
            total = self.piece(self.me, half)[...].astype(F32) + self.final[0, half].astype(F32) + self.final[1, half].astype(F32)
            put(half, total.astype(BF16))
        for k in range(6):
            self.copy(k).wait_send()


def forward_body(x_ref, dy_ref, wg_ref, wu_ref, wd_ref, gate_ref, up_ref, hid_ref, at_ref, h_ref, a2_ref, a2t_ref, dyt_ref, hid):
    x = x_ref[...].astype(F32)
    a = (x * scale_of(x)).astype(BF16)
    for j in range(wg_ref.shape[1] // CHUNK):
        at = slice(j * CHUNK, (j + 1) * CHUNK)
        gate, up = dot(a, wg_ref[:, at]), dot(a, wu_ref[:, at])
        gate_ref[j], up_ref[j] = gate, up
        hid[:, at] = hid_ref[j] = (gate * jax.nn.sigmoid(gate) * up).astype(BF16)
    h = (x + dot(hid[...], wd_ref[...]).astype(BF16).astype(F32)).astype(BF16)
    h_ref[...] = h
    wide = h.astype(F32)
    a2 = (wide * scale_of(wide)).astype(BF16)
    a2_ref[...] = a2
    a2t_ref[...] = a2.T
    at_ref[...] = a.T
    dyt_ref[...] = dy_ref[...].T


def forward(x, dy, wg, wu, wd, layer, tile=512):
    tokens, d = x.shape
    ff = wg.shape[2]
    chunks = ff // CHUNK
    rows = pl.BlockSpec((tile, d), lambda i: (i, 0))
    columns = pl.BlockSpec((d, tile), lambda i: (0, i))
    kept = pl.BlockSpec((chunks, tile, CHUNK), lambda i: (0, i, 0))
    flat, turned = jax.ShapeDtypeStruct((tokens, d), BF16), jax.ShapeDtypeStruct((d, tokens), BF16)
    by_chunk = (chunks, tokens, CHUNK)
    return pl.pallas_call(
        forward_body,
        grid=(tokens // tile,),
        in_specs=[rows, rows, whole((d, ff), layer), whole((d, ff), layer), whole((ff, d), layer)],
        out_specs=[kept, kept, kept, columns, rows, rows, columns, columns],
        out_shape=[*(jax.ShapeDtypeStruct(by_chunk, t) for t in (F32, F32, BF16)), turned, flat, flat, turned, turned],
        scratch_shapes=[pltpu.VMEM((tile, ff), BF16)],
        compiler_params=pltpu.CompilerParams(vmem_limit_bytes=VMEM_LIMIT),
        cost_estimate=pl.CostEstimate(flops=6 * tokens * d * ff, bytes_accessed=16 * tokens * d, transcendentals=tokens * ff),
        name="forward",
    )(x, dy, wg, wu, wd)


def of(n):
    return lambda i: (2 * i) % n


def aligned(start, length, unit):
    return pl.ds(pl.multiple_of(start, unit), length)


def pair_job(ref, slot, landed, final, send, recv):
    part = landed.shape[-2]
    return Scatter(lambda owner, half: ref.at[:, aligned((2 * owner + half) * part, part, 32), :], landed.at[slot], final.at[slot], send.at[slot], recv.at[slot])


def put_pair(gg, gu, layer, chunk):
    def put(half, value):
        part = value.shape[1]
        at = (*layer, slice(half * part, (half + 1) * part), aligned(chunk * CHUNK, CHUNK, CHUNK))
        gg[at], gu[at] = value[0], value[1]

    return put


def down_job(ref, start, slot, landed, final, send, recv):
    part = landed.shape[-2]
    return Scatter(lambda owner, half: ref.at[aligned(start(owner) + half * part, part, 16), :], landed.at[slot], final.at[slot], send.at[slot], recv.at[slot])


def put_down(gd, layer, start):
    def put(half, value):
        part = value.shape[0]
        gd[(*layer, aligned(start + half * part, part, 16), slice(None))] = value

    return put


def left_over(owner, b, share):
    short = 2 * CHUNK - share
    return b * short + (1 - (owner - b + 3) // 4) * CHUNK


def gradients_of(gate, up, dhid):
    sig = jax.nn.sigmoid(gate)
    silu = gate * sig
    return (silu * up).astype(BF16), (dhid * up * (sig + silu * (1 - sig))).astype(BF16), (dhid * silu).astype(BF16)


def squares_of(ref, layer):
    def add(r, squares):
        part = ref[layer, pl.ds(pl.multiple_of(r * 16, 16), 16), :].astype(F32)
        return squares + part * part

    return jnp.sum(lax.fori_loop(0, ref.shape[1] // 16, add, jnp.zeros((16, ref.shape[2]), F32)))


def last_body(tile, unroll, *refs):
    a_in, at_in, dy_in, dyt_in, wg_ref, wu_ref, wd_ref, h_ref, dh_ref, dht_ref, gg, gu, gd, pair, down, a_ref, at_ref, dy_ref, dyt_ref, loads, gw, uw, dw, *rest = refs
    (*pairs, landed1, final1, send1, recv1, da, h, h_sem, out_sem) = rest
    tokens, d = dy_ref.shape
    share = gd.shape[0]
    i, chunks = pl.program_id(0), pl.num_programs(0)
    order = of(chunks)
    me, right, left, far = ring()
    n_tiles = tokens // tile
    wg, wu, wd = wg_ref[...], wu_ref[...], wd_ref[...]
    wgu = jnp.concatenate([wg, wu], 1)

    def own(number):
        return pair_job(pair, number, *pairs)

    def evens():
        return down_job(down, lambda owner: owner * 2 * CHUNK, 0, landed1, final1, send1, recv1)

    def rows_of(t):
        return aligned(t * tile, tile, tile)

    def load(t):
        by_rows, by_columns = (rows_of(t), slice(None)), (slice(None), rows_of(t))
        arrays = (dy_in, dy_ref, by_rows), (a_in, a_ref, by_rows), (at_in, at_ref, by_columns), (dyt_in, dyt_ref, by_columns)
        return [pltpu.make_async_copy(src.at[at], dst.at[at], loads.at[k, t]) for k, (src, dst, at) in enumerate(arrays)]

    def fetch(t, slot):
        return pltpu.make_async_copy(h_ref.at[rows_of(t), :], h.at[slot], h_sem.at[slot])

    def hand_on(t):
        by_rows, by_columns = (rows_of(t), slice(None)), (slice(None), rows_of(t))
        return [
            pltpu.make_async_copy(dy_ref.at[by_rows], dh_ref.at[by_rows], out_sem.at[0, t]),
            pltpu.make_async_copy(dyt_ref.at[by_columns], dht_ref.at[by_columns], out_sem.at[1, t]),
        ]

    def step(t, ends=False):
        rows = rows_of(t)
        a, dy = a_ref[rows, :], dy_ref[rows, :]
        hid, dgate, dup = gradients_of(dot(a, wg), dot(a, wu), dot_t(dy, wd).astype(BF16).astype(F32))
        at, dyt = at_ref[:, rows], dyt_ref[:, rows]
        dw[...] += dot(dyt, hid)
        da_t = dot_t(jnp.concatenate([dgate, dup], 1), wgu)
        uw[...] += dot(at, dup)
        gw[...] += dot(at, dgate)
        if not ends:
            da[rows, :] += da_t
        else:
            wide = h[t % 2].astype(F32)
            scale = scale_of(wide)
            back = (da[rows, :] + da_t).astype(BF16).astype(F32)
            coefficient = jnp.sum(back * wide, -1, keepdims=True) * (scale * scale * scale) * (1.0 / wide.shape[1])
            through = (back * scale - wide * coefficient).astype(BF16)
            dh = (dy.astype(F32) + through.astype(F32)).astype(BF16)
            dy_ref[rows, :] = dh
            dyt_ref[:, rows] = dh.T

    def steps(start, stop):
        def some(m, carry):
            @pl.when(i == 0)
            def _():
                for k in range(unroll):
                    for copy in load(m * unroll + k):
                        copy.wait()

            for k in range(unroll):
                step(m * unroll + k)
            return carry

        def some_last(t, carry):
            fetch(t, t % 2).wait()

            @pl.when(t + 1 < n_tiles)
            def _():
                fetch(t + 1, (t + 1) % 2).start()

            @pl.when(t > 0)
            def _():
                for copy in hand_on(t - 1):
                    copy.start()

            step(t, ends=True)
            return carry

        @pl.when(i < chunks - 1)
        def _():
            lax.fori_loop(start // unroll, stop // unroll, some, 0)

        @pl.when(i == chunks - 1)
        def _():
            if start == 0:
                fetch(0, 0).start()
            lax.fori_loop(start, stop, some_last, 0)

    for total in (gw, uw, dw):
        total[...] = jnp.zeros_like(total)

    def clear(t, carry):
        da[rows_of(t), :] = jnp.zeros((tile, d), F32)
        return carry

    @pl.when(i == 0)
    def _():
        for t in range(n_tiles):
            for copy in load(t):
                copy.start()
        lax.fori_loop(0, n_tiles, clear, 0)
        meet((right, left))

    @pl.when(i > 0)
    def _():
        own(i - 1).start()

    steps(0, n_tiles // 2)

    @pl.when(i > 0)
    def _():
        own(i - 1).middle()

    @pl.when(i == 4)
    def _():
        evens().start()

    @pl.when(i == 5)
    def _():
        evens().middle()

    @pl.when(i == 6)
    def _():
        evens().finish(put_down(gd, (), me * (2 * CHUNK - share)))

    steps(n_tiles // 2, n_tiles)

    @pl.when(i > 0)
    def _():
        own(i - 1).finish(put_pair(gg, gu, (), order(i - 1)))

    pair[0] = gw[...].astype(BF16)
    pair[1] = uw[...].astype(BF16)
    down[aligned(order(i) * CHUNK, CHUNK, CHUNK), :] = dw[...].astype(BF16).T

    @pl.when(i == chunks - 1)
    def _():
        for copy in hand_on(n_tiles - 1):
            copy.start()
        for t in range(n_tiles):
            for copy in hand_on(t):
                copy.wait()


def first_body(tile, unroll, *refs):
    gate_in, up_in, hid_ref, at_in, dy_in, dyt_in, wd_ref, gg_in, gu_in, gd_in, pair_in, down_hbm, gg, gu, gd, squares, pair, down, down_in, kept, kept_sem, g_sem, at_ref, dy_ref, dyt_ref, loads, gw, uw, by, *rest = refs
    pairs, downs, leftovers = rest[:4], rest[4:8], rest[8:]
    tokens, d = dy_ref.shape
    share = gd.shape[-2]
    i, chunks = pl.program_id(0), down.shape[0] // CHUNK
    n = i - chunks
    me, right, left, far = ring()
    n_tiles = tokens // tile
    runs = downs[0].shape[0]
    run = share // runs

    def held(row):
        return row // (2 * CHUNK) * CHUNK + row % CHUNK

    def odd_chunks():
        return [
            pltpu.make_async_copy(down_hbm.at[(2 * b + 1) * CHUNK : (2 * b + 2) * CHUNK, :], down_in.at[b * CHUNK : (b + 1) * CHUNK, :], g_sem.at[3 + b])
            for b in range(chunks // 2)
        ]

    def before():
        jobs = [(pair_job(pair_in, chunks, *pairs), put_pair(gg, gu, (1,), of(chunks)(chunks - 1)))]
        for b in range(3):
            start = functools.partial(left_over, b=b, share=share)
            jobs.append((down_job(down_in, lambda owner, start=start: held(owner * share + start(owner)), b, *leftovers), put_down(gd, (1,), start(me))))
        return jobs

    def own(number):
        return pair_job(pair.at[number % 3], number, *pairs), put_pair(gg, gu, (0,), number)

    def rows_job(number):
        return down_job(down, lambda owner: owner * share + number * run, number, *downs), put_down(gd, (0,), number * run)

    def rows_of(t):
        return aligned(t * tile, tile, tile)

    def load(k, t):
        by_rows, by_columns = (rows_of(t), slice(None)), (slice(None), rows_of(t))
        src, dst, at = ((dyt_in, dyt_ref, by_columns), (dy_in, dy_ref, by_rows), (at_in, at_ref, by_columns))[k]
        return pltpu.make_async_copy(src.at[at], dst.at[at], loads.at[k, t])

    def keep(number):
        return [pltpu.make_async_copy(src.at[number], kept.at[number % 2, k], kept_sem.at[number % 2, k]) for k, src in enumerate((gate_in, up_in))]

    def g_before():
        return [pltpu.make_async_copy(src, dst.at[1], g_sem.at[k]) for k, (src, dst) in enumerate(((gg_in, gg), (gu_in, gu), (gd_in, gd)))]

    @pl.when(i == 0)
    def _():
        for copy in odd_chunks() + [load(0, t) for t in range(n_tiles)] + g_before() + [load(k, t) for t in range(n_tiles) for k in (1, 2)] + keep(0):
            copy.start()
        meet((right, left))
        for copy in odd_chunks():
            copy.wait()
        for job, _ in before():
            job.start()

    @pl.when(i == 4)
    def _():
        before()[0][0].middle()

    @pl.when(i == 6)
    def _():
        for copy in g_before():
            copy.wait()
        jobs = before()
        for job, _ in jobs[1:]:
            job.middle()
        jobs[0][0].finish(jobs[0][1])

    @pl.when(i == chunks + 1)
    def _():
        for job, put in before()[1:]:
            job.finish(put)

    @pl.when(n < 0)
    def _():
        gw[...] = jnp.zeros_like(gw)

        def some(t, carry):
            @pl.when(i == 0)
            def _():
                for k in range(unroll):
                    load(0, t * unroll + k).wait()

            rows = pl.ds(pl.multiple_of(t * tile * unroll, tile * unroll), tile * unroll)
            gw[...] += dot(dyt_ref[:, rows], hid_ref[rows, :])
            return carry

        lax.fori_loop(0, n_tiles // unroll, some, 0)
        down[aligned(i * CHUNK, CHUNK, CHUNK), :] = gw[...].astype(BF16).T

    @pl.when(n >= 1)
    def _():
        own(n - 1)[0].start()

    for b in range(2):

        @pl.when(n == b)
        def _():
            rows_job(b)[0].start()

    @pl.when(n >= 2)
    def _():
        own(n - 2)[0].middle()

    for b in range(2):

        @pl.when(n == b + 2)
        def _():
            rows_job(b)[0].middle()

    @pl.when(n >= 3)
    def _():
        job, put = own(n - 3)
        job.finish(put)

    for b in range(2):

        @pl.when(n == b + 4)
        def _():
            job, put = rows_job(b)
            job.finish(put)

    @pl.when(n == 4)
    def _():
        squares[...] = jnp.full(squares.shape, sum(squares_of(ref, 1) for ref in (gg, gu, gd)), F32)

    @pl.when(n >= 0)
    def _():
        @pl.when(n + 1 < chunks)
        def _():
            for copy in keep(n + 1):
                copy.start()

        gw[...] = jnp.zeros_like(gw)
        uw[...] = jnp.zeros_like(uw)
        wd = wd_ref[...]
        for copy in keep(n):
            copy.wait()
        slot = n % 2

        def some(m, carry):
            @pl.when(n == 0)
            def _():
                for k in range(unroll):
                    for which in (1, 2):
                        load(which, m * unroll + k).wait()

            for k in range(unroll):
                rows = rows_of(m * unroll + k)
                dhid = dot_t(dy_ref[rows, :], wd).astype(BF16).astype(F32)
                _, dgate, dup = gradients_of(kept[slot, 0, rows, :], kept[slot, 1, rows, :], dhid)
                by[0, k * tile : (k + 1) * tile, :] = dgate
                by[1, k * tile : (k + 1) * tile, :] = dup
            at = at_ref[:, aligned(m * unroll * tile, unroll * tile, unroll * tile)]
            gw[...] += dot(at, by[0])
            uw[...] += dot(at, by[1])
            return carry

        lax.fori_loop(0, n_tiles // unroll, some, 0)
        pair[n % 3, 0] = gw[...].astype(BF16)
        pair[n % 3, 1] = uw[...].astype(BF16)

    @pl.when(n == chunks - 1)
    def _():
        ends = [own(chunks - 3 + k) for k in range(3)]
        ends[2][0].start()
        ends[1][0].middle()
        ends[0][0].finish(ends[0][1])
        ends[2][0].middle()
        for job, put in ends[1:]:
            job.finish(put)
        squares[...] += sum(squares_of(ref, 0) for ref in (gg, gu, gd))


def scatter_scratch(jobs, *half):
    dma = pltpu.SemaphoreType.DMA
    return [pltpu.VMEM((jobs, 2, *half), BF16), pltpu.VMEM((jobs, 2, 2, *half), BF16), dma((jobs, 6)), dma((jobs, 6))]


def shares(w, group):
    _, d, ff = w[0].shape
    return [(d // group, ff), (d // group, ff), (ff // group, d)]


def backward_last(a, at, dy, dyt, w, layer, h, group, tile=512, unroll=1):
    tokens, d = dy.shape
    _, _, ff = w[0].shape
    chunks = ff // CHUNK
    by_columns = pl.BlockSpec((None, d, CHUNK), lambda i: (layer, 0, of(chunks)(i)))
    by_rows = pl.BlockSpec((None, CHUNK, d), lambda i: (layer, of(chunks)(i), 0))
    shapes = shares(w, group) + [(2, d, CHUNK), (ff, d)]
    dma = pltpu.SemaphoreType.DMA
    scratch = [pltpu.VMEM((tokens, d), BF16), pltpu.VMEM((d, tokens), BF16)] * 2 + [dma((4, tokens // tile))]
    scratch += [pltpu.VMEM((d, CHUNK), F32)] * 3
    scratch += scatter_scratch(chunks - 1, 2, d // group // 2, CHUNK) + scatter_scratch(1, CHUNK // 2, d)
    scratch += [pltpu.VMEM((tokens, d), F32), pltpu.VMEM((2, tile, d), BF16), dma((2,)), dma((2, tokens // tile))]
    return pl.pallas_call(
        functools.partial(last_body, tile, unroll),
        grid=(chunks,),
        in_specs=[ANY] * 4 + [by_columns, by_columns, by_rows, ANY],
        out_specs=[ANY, ANY] + [whole(s) for s in shapes],
        out_shape=[jax.ShapeDtypeStruct(s, BF16) for s in ((tokens, d), (d, tokens), *shapes)],
        scratch_shapes=scratch,
        compiler_params=pltpu.CompilerParams(vmem_limit_bytes=VMEM_LIMIT, collective_id=1, has_side_effects=True),
        cost_estimate=pl.CostEstimate(flops=16 * tokens * d * ff, bytes_accessed=16 * tokens * d, transcendentals=tokens * ff),
        name="backward_last",
    )(a, at, dy, dyt, *w, h)


def backward_first(gate, up, hid, at, dy, dyt, w, layer, before, group, tile=512, unroll=4):
    tokens, d = dy.shape
    layers, _, ff = w[0].shape
    chunks = ff // CHUNK
    by_chunk = pl.BlockSpec((None, tokens, CHUNK), lambda i: (jnp.minimum(i, chunks - 1), 0, 0))
    by_rows = pl.BlockSpec((None, CHUNK, d), lambda i: (layer, jnp.maximum(i - chunks, 0), 0))
    shapes = [(layers, *s) for s in shares(w, group)]
    dma = pltpu.SemaphoreType.DMA
    short = 2 * CHUNK - ff // group
    scratch = [pltpu.VMEM((3, 2, d, CHUNK), BF16), pltpu.VMEM((ff, d), BF16), pltpu.VMEM((chunks // 2 * CHUNK, d), BF16)]
    scratch += [pltpu.VMEM((2, 2, tokens, CHUNK), F32), dma((2, 2)), dma((3 + chunks // 2,))]
    scratch += [pltpu.VMEM((d, tokens), BF16), pltpu.VMEM((tokens, d), BF16), pltpu.VMEM((d, tokens), BF16), dma((3, tokens // tile))]
    scratch += [pltpu.VMEM((d, CHUNK), F32)] * 2 + [pltpu.VMEM((2, unroll * tile, CHUNK), BF16)]
    scratch += scatter_scratch(chunks + 1, 2, d // group // 2, CHUNK) + scatter_scratch(2, ff // group // 4, d) + scatter_scratch(3, short // 2, d)
    return pl.pallas_call(
        functools.partial(first_body, tile, unroll),
        grid=(2 * chunks,),
        in_specs=[ANY, ANY, by_chunk] + [ANY] * 3 + [by_rows] + [ANY] * 3 + [whole((2, d, CHUNK)), ANY],
        out_specs=[whole(s) for s in (*shapes, (8, 128))],
        out_shape=[jax.ShapeDtypeStruct(s, BF16) for s in shapes] + [jax.ShapeDtypeStruct((8, 128), F32)],
        scratch_shapes=scratch,
        compiler_params=pltpu.CompilerParams(vmem_limit_bytes=VMEM_LIMIT, collective_id=2, has_side_effects=True),
        cost_estimate=pl.CostEstimate(flops=8 * tokens * d * ff, bytes_accessed=16 * tokens * d, transcendentals=tokens * ff),
        name="backward_first",
    )(gate, up, hid, at, dy, dyt, w[2], *before)


def adamw(w, m, v, g):
    m = 0.9 * m + 0.1 * g
    v = 0.95 * v + 0.05 * g * g
    step = m * lax.rsqrt(v + 1e-8) + 0.1 * w
    return (w - 0.02 * step).astype(BF16), m, v


def update_body(count, *refs):
    mine, *refs = refs
    g_in, w, m, v, new_w, new_m, new_v, g = (refs[k : k + 3] for k in range(0, 24, 3))
    sums, norm_send, norm_recv, load, send, recv = refs[24:]
    me, right, left, far = ring()
    layers = g[0].shape[0]
    loads = {}

    def fetch(which, k, layer, src, dst, at):
        loads[k, layer, which] = pltpu.make_async_copy(src[k].at[at], dst[k].at[at], load.at[k, layer, which])
        loads[k, layer, which].start()

    parts = [(k, layer) for k in range(3) for layer in range(layers)]
    for k, layer in parts:
        fetch(3, k, layer, g_in, g, layer)
        fetch(0, k, layer, w, new_w, (layer, pl.ds(pl.multiple_of(me * g[k].shape[1], 32), g[k].shape[1])))
        fetch(1, k, layer, m, new_m, layer)
        fetch(2, k, layer, v, new_v, layer)
    meet((right, left, far))
    sums[me] = mine[...]
    tells = [remote(mine, sums.at[me], norm_send.at[n], norm_recv.at[n], to) for n, to in enumerate((right, left, far))]
    for tell in tells:
        tell.start()
    for tell in tells:
        tell.wait()
    squares = sum(sums[n] for n in range(sums.shape[0]))
    factor = jnp.minimum(1.0, 0.5 * lax.rsqrt(squares / count + 1e-30))[0:1, 0:1]

    copies = []
    for k in range(3):
        size, rows = g[k].shape[1], 32
        half = size // 2
        for layer in range(layers):
            for which in range(4):
                loads[k, layer, which].wait()

            def change(r, carry):
                at = (layer, pl.ds(pl.multiple_of(r * rows, rows), rows), slice(None))
                own = (layer, pl.ds(pl.multiple_of(me * size + r * rows, rows), rows), slice(None))
                new = adamw(new_w[k][own].astype(F32), new_m[k][at], new_v[k][at], g[k][at].astype(F32) * factor)
                new_w[k][own], new_m[k][at], new_v[k][at] = new
                return carry

            lax.fori_loop(0, size // rows, change, 0)

            def block(owner, start, length):
                return new_w[k].at[layer, pl.ds(pl.multiple_of(owner * size + start, 32), length), :]

            s, r = send.at[k, layer], recv.at[k, layer]
            direct = [remote(block(me, 0, size), block(me, 0, size), s.at[n], r.at[n], to) for n, to in enumerate((right, left))]
            on = [
                remote(block(left, 0, half), block(left, 0, half), s.at[2], r.at[2], right),
                remote(block(right, half, half), block(right, half, half), s.at[3], r.at[3], left),
            ]
            for copy in direct:
                copy.start()
            copies.append((direct, on))
    for direct, on in copies:
        for first, second in zip(direct, on, strict=True):
            first.wait_recv()
            second.start()
    for direct, on in copies:
        for copy in on:
            copy.wait()
        for copy in direct:
            copy.wait_send()


def update(squares, g, w, m, v):
    count = sum(t.size for t in w)
    layers = w[0].shape[0]
    shapes = [pltpu.VMEM(t.shape, t.dtype) for t in (*w, *m, *v)]
    dma = pltpu.SemaphoreType.DMA
    group = w[0].shape[1] // m[0].shape[1]
    vmem = pl.BlockSpec(memory_space=pltpu.VMEM)
    return pl.pallas_call(
        functools.partial(update_body, count),
        in_specs=[vmem] + [ANY] * 12,
        out_specs=[vmem] * 9,
        out_shape=shapes,
        scratch_shapes=[pltpu.VMEM(t.shape, BF16) for t in m]
        + [pltpu.VMEM((group, 8, 128), F32), dma((3,)), dma((3,))]
        + [dma((3, layers, 4)), dma((3, layers, 4)), dma((3, layers, 4))],
        compiler_params=pltpu.CompilerParams(vmem_limit_bytes=28_000_000, collective_id=3, has_side_effects=True),
        name="update",
    )(squares, *g, *w, *m, *v)


def deliver_body(*refs):
    copies = [pltpu.make_async_copy(refs[k], refs[9 + k], refs[18].at[k]) for k in range(9)]
    for copy in copies:
        copy.start()
    for copy in copies:
        copy.wait()


def deliver(arrays):
    arrays = [pltpu.with_memory_space_constraint(t, pltpu.VMEM) for t in arrays]
    return pl.pallas_call(
        deliver_body,
        in_specs=[pl.BlockSpec(memory_space=pltpu.VMEM)] * 9,
        out_specs=[ANY] * 9,
        out_shape=[jax.ShapeDtypeStruct(t.shape, t.dtype) for t in arrays],
        scratch_shapes=[pltpu.SemaphoreType.DMA((9,))],
        compiler_params=pltpu.CompilerParams(vmem_limit_bytes=28_000_000),
        name="deliver",
    )(*arrays)


def solution(mesh):
    group = mesh.shape["dp"]

    def step(x, dy, *arrays):
        w, m, v = (arrays[i : i + 3] for i in (0, 3, 6))
        x, dy = x[0], dy[0]
        gate, up, hid, a1t, h1, a2, a2t, dyt = forward(x, dy, *w, 0)
        dh, dht, *before = backward_last(a2, a2t, dy, dyt, w, 1, h1, group)
        *g, squares = backward_first(gate, up, hid, a1t, dh, dht, w, 0, before, group)
        return tuple(deliver(update(squares, g, w, m, v)))

    sequence, rows = P(("rep", "dp"), None, None), P(None, "dp", None)
    return jax.shard_map(
        step,
        mesh=mesh,
        in_specs=(sequence,) * 2 + (P(),) * 3 + (rows,) * 6,
        out_specs=(P("rep", None, None),) * 3 + (P("rep", "dp", None),) * 6,
        check_vma=False,
    )
```
